32 devices in a mesh: dp: 8 (over y, x, core), mp: 4 (over z).
Axes of the slice: x: 2, y: 2, z: 4, core: 2. Of those that a mesh axis runs over, the one named last changes fastest.
Arguments:
- tokens: bfloat16 [8192, 2048], P('dp'), may hold values from -6 to 6
- doc_lengths: int32 [8, 8], P('dp'), may hold values from 1 to 512, 1024 in all within a row
- slot_live: int32 [36], P('mp'), may hold values from 0 to 1, as said below
- attn_gain: bfloat16 [2048], replicated, may hold values from 0.5 to 1.5
- w_query: bfloat16 [2048, 1536], P(None, 'mp'), may hold values from -0.125 to 0.125
- w_keyval: bfloat16 [2048, 768], replicated, may hold values from -0.125 to 0.125
- q_gain: bfloat16 [64], replicated, may hold values from 0.099609375 to 1.8984375
- k_gain: bfloat16 [64], replicated, may hold values from 0.099609375 to 1.8984375
- w_out: bfloat16 [1536, 2048], P('mp'), may hold values from -0.625 to 0.625
- ffn_gain: bfloat16 [2048], replicated, may hold values from 0.5 to 1.5
- w_gate: bfloat16 [2048, 4608], P(None, 'mp'), may hold values from -0.125 to 0.125
- w_up: bfloat16 [2048, 4608], P(None, 'mp'), may hold values from -0.125 to 0.125
- w_down: bfloat16 [4608, 2048], P('mp'), may hold values from -0.09375 to 0.09375
- out_grad: bfloat16 [8192, 2048], P('dp'), may hold values from -6 to 6
Outputs:
- block_out: bfloat16 [8192, 2048], P(('dp', 'mp'))
- grad_tokens: float32 [8192, 2048], P(('dp', 'mp'))
- grad_attn_gain: float32 [2048], replicated
- grad_query: float32 [2048, 1536], P('dp', 'mp')
- grad_keyval: float32 [2048, 768], P(('dp', 'mp'))
- grad_q_gain: float32 [64], replicated
- grad_k_gain: float32 [64], replicated
- grad_out_proj: float32 [1536, 2048], P('mp', 'dp')
- grad_ffn_gain: float32 [2048], replicated
- grad_gate: float32 [2048, 4608], P('dp', 'mp')
- grad_up: float32 [2048, 4608], P('dp', 'mp')
- grad_down: float32 [4608, 2048], P('mp', 'dp')
The draws below stay inside these ranges and needn't reach their ends.
Inputs may be any that keep to these rules, and one draw needn't show every extreme that they name: `doc_lengths`: each row's 8 lengths sum to 1024, and one of them is 512. `slot_live`: the 9 slots of each index of mp hold 34 // 4 or 34 // 4 + 1 live ones, 34 live in all; which slots and which indices hold more varies.
All inputs are finite; a program needn't handle non-finite values.
Results may differ from the reference program's by a relative error of at most 0.018.
Values may be sent and summed in bfloat16 or wider, within the bound.
A program may use at most 192 MiB of HBM per device.

```python
import math
import jax
import jax.numpy as jnp
import numpy as np
from jax import lax

D = 2048
HQ = 24
KV = 6
HD = 64
FF_TILES = 34
TILE = 128
TOK_DEV = 1024
NDOC = 8
DOC_MOST = 512
SLOTS = 9
FFS = 4608
FF = 4352
TOKENS = 8192
N_DP = 8
N_MP = 4


def draw_slot_live(key, part):
    key_devices, key_slots = jax.random.split(key)
    dev_order = jax.random.permutation(key_devices, N_MP)
    live_count = FF_TILES // N_MP + (dev_order < FF_TILES % N_MP).astype(jnp.int32)
    slot_keys = jax.random.split(key_slots, N_MP)
    slot_ranks = jax.vmap(lambda one_key: jax.random.permutation(one_key, SLOTS))(slot_keys)
    return (slot_ranks < live_count[:, None]).astype(jnp.int32).reshape(N_MP * SLOTS)


def raised(values, stream_key, source, target, parts, factor):
    def block_of(position):
        return (jnp.arange(values.shape[position]) // (values.shape[position] // parts)).reshape((-1,) + (1,) * (values.ndim - 1 - position))

    one_side = jax.random.permutation(stream_key, parts)[block_of(target)]
    other_side = (block_of(target) + parts // 2) % parts
    return jnp.where((block_of(source) == one_side) | (block_of(source) == other_side), factor * values, values)


def level_of(stream_key, dims, cuts, low, high):
    level = 1.0
    for dim, blocks in cuts:
        steps = jax.random.uniform(jax.random.fold_in(jax.random.fold_in(stream_key, 6), dim), (blocks,), jnp.float32, low / len(cuts), high / len(cuts))
        level = level * jnp.repeat(jnp.exp(steps), dims[dim] // blocks).reshape((-1,) + (1,) * (len(dims) - 1 - dim))
    return level


def length_profile(number_of, total, bound, lean):
    loads = [(1 << 20) // math.isqrt(grade ** lean) + 1 for grade in range(2, number_of + 1)]
    rest, counts = total - bound - (number_of - 1), [1] * (number_of - 1)
    while rest > 0:
        candidates = [i for i in range(number_of - 1) if counts[i] < bound]
        pool, budget = sum([loads[i] for i in candidates]), rest
        for i in candidates:
            addition = min(bound - counts[i], max(1, budget * loads[i] // pool), rest)
            counts[i] = counts[i] + addition
            rest = rest - addition
    return np.array([bound] + counts)


def uneven(key, count, total, bound, skew):
    if count == 2:
        one = jax.random.randint(key, (), max(1, total - bound), min(bound, total - 1) + 1)
        return jnp.stack([one, total - one])
    tallies = jnp.asarray(length_profile(count, total, bound, skew), jnp.int32)
    pairs = (count - 1) // 2
    source_of, receiver = tallies[1:1 + 2 * pairs:2], tallies[2:2 + 2 * pairs:2]
    room = jnp.minimum(source_of - 1, bound - receiver)
    shifted = jax.random.randint(jax.random.fold_in(key, 1), (pairs,), 0, 1 << 20) % (room + 1)
    tallies = tallies.at[1:1 + 2 * pairs:2].set(source_of - shifted).at[2:2 + 2 * pairs:2].set(receiver + shifted)
    return tallies[jax.random.permutation(jax.random.fold_in(key, 2), count)]


def gaussian(stream_key, shape, deviation, most, cuts=(), kind=jnp.bfloat16):
    array = deviation * jax.random.normal(stream_key, shape, jnp.float32)
    if cuts:
        array = array * level_of(stream_key, shape, cuts, -0.22, 0.18)
    return jnp.clip(array, -most, most).astype(kind)


def gaussian_with(own_key, dims, scale, bound, cuts, heavy, held_as=jnp.bfloat16):
    entries = scale * jax.random.normal(own_key, dims, jnp.float32)
    if cuts:
        entries = entries * level_of(own_key, dims, cuts, -0.22, 0.18)
    return jnp.clip(raised(entries, jax.random.fold_in(own_key, 3), *heavy), -bound, bound).astype(held_as)


def setup_inputs(seed: int = 0) -> dict:
    streams_of = jax.random.split(jax.random.key(seed), 15)
    tokens = gaussian(streams_of[0], (TOKENS, D), 1.0, 6.0, ((0, 8),))
    doc_lengths = jax.vmap(lambda own: uneven(own, NDOC, TOK_DEV, DOC_MOST, 2))(jax.random.split(streams_of[1], N_DP)).reshape((N_DP, NDOC)).astype(jnp.int32)
    slot_live = draw_slot_live(jax.random.fold_in(streams_of[14], 71), 0)
    attn_gain = jnp.clip(1.0 + 0.1 * jax.random.normal(streams_of[3], (D,), jnp.float32), 0.5, 1.5).astype(jnp.bfloat16)
    w_query = gaussian(streams_of[4], (D, HQ * HD), D ** -0.5, 0.125, ((1, 4),))
    w_keyval = gaussian(streams_of[5], (D, 2 * KV * HD), D ** -0.5, 0.125)
    q_gain = jnp.clip(1.0 + 0.18 * jax.random.normal(streams_of[6], (HD,), jnp.float32), 0.099609375, 1.8984375).astype(jnp.bfloat16)
    k_gain = jnp.clip(1.0 + 0.18 * jax.random.normal(streams_of[7], (HD,), jnp.float32), 0.099609375, 1.8984375).astype(jnp.bfloat16)
    w_out = gaussian(streams_of[8], (HQ * HD, D), (HQ * HD // 16) ** -0.5, 0.625, ((0, 4),))
    ffn_gain = jnp.clip(1.0 + 0.1 * jax.random.normal(streams_of[9], (D,), jnp.float32), 0.5, 1.5).astype(jnp.bfloat16)
    w_gate = gaussian(streams_of[10], (D, FFS), D ** -0.5, 0.125, ((1, 4),))
    w_up = gaussian(streams_of[11], (D, FFS), D ** -0.5, 0.125, ((1, 4),))
    w_down = gaussian(streams_of[12], (FFS, D), FF ** -0.5, 0.09375, ((0, 4),))
    out_grad = gaussian_with(streams_of[13], (TOKENS, D), 1.0, 6.0, ((0, 8),), (0, 1, 8, 2.0))
    return {"tokens": tokens, "doc_lengths": doc_lengths, "slot_live": slot_live, "attn_gain": attn_gain, "w_query": w_query, "w_keyval": w_keyval, "q_gain": q_gain, "k_gain": k_gain, "w_out": w_out, "ffn_gain": ffn_gain, "w_gate": w_gate, "w_up": w_up, "w_down": w_down, "out_grad": out_grad}


EPSILON = 1e-06
MASKED = -1000000000.0
ROPE_BASE = 10000.0
HIGHEST_PREC = lax.Precision.HIGHEST

@jax.custom_vjp
def low(v):
    return lax.optimization_barrier(v.astype(jnp.bfloat16)).astype(jnp.float32)

@jax.custom_vjp
def low_back(v):
    return v

def low_keep(v):
    return (low(v), None)

def low_pass(kept, grad):
    return (grad,)

def back_keep(v):
    return (v, None)

def back_low(kept, grad):
    return (low(grad),)
low.defvjp(low_keep, low_pass)
low_back.defvjp(back_keep, back_low)

def normalize(raw_in):
    return raw_in * lax.rsqrt(lax.optimization_barrier(jnp.mean(raw_in * raw_in, axis=-1, keepdims=True)) + EPSILON)

def rotate(values, cosine_tab, sine_tab, sign):
    half_size = values.shape[-1] // 2
    first_half = values[..., :half_size]
    second_half = values[..., half_size:]
    return jnp.concatenate([first_half * cosine_tab - sign * second_half * sine_tab, second_half * cosine_tab + sign * first_half * sine_tab], axis=-1)

def doc_layout(lengths, row_count):
    doc_ends = jnp.cumsum(lengths).astype(jnp.int32)
    token_index = jnp.arange(row_count, dtype=jnp.int32)
    past_end = (token_index[:, None] >= doc_ends[None, :]).astype(jnp.int32)
    doc_id = lax.optimization_barrier(jnp.sum(past_end, axis=1)).astype(jnp.int32)
    doc_pos = token_index - lax.optimization_barrier(jnp.sum(past_end * lengths[None, :], axis=1)).astype(jnp.int32)
    return (doc_id, doc_pos, token_index)

def rope_table(doc_pos, head_size):
    rope_freq = jnp.exp(jnp.arange(head_size // 2, dtype=jnp.float32) * (-2.0 * math.log(ROPE_BASE) / head_size))
    rope_angle = doc_pos.astype(jnp.float32)[:, None] * rope_freq[None, :]
    return (jnp.cos(rope_angle)[:, None, :], jnp.sin(rope_angle)[:, None, :])

def sequence(x_seq, lengths, live_cols, gain_one, w_query, w_keyval, q_gain, k_gain, w_out, gain_two, w_gate, w_up, w_down):
    doc_id, doc_pos, token_index = doc_layout(lengths, TOK_DEV)
    cosine_tab, sine_tab = rope_table(doc_pos, HD)
    xn_one = low(normalize(x_seq) * gain_one)
    q_raw = low_back(jnp.dot(xn_one, w_query, precision=HIGHEST_PREC)).reshape(TOK_DEV, HQ, HD)
    kv_all = jnp.dot(xn_one, w_keyval, precision=HIGHEST_PREC)
    k_raw = low_back(jnp.repeat(kv_all[:, :KV * HD].reshape(TOK_DEV, KV, HD), HQ // KV, axis=1))
    v_raw = low_back(jnp.repeat(kv_all[:, KV * HD:].reshape(TOK_DEV, KV, HD), HQ // KV, axis=1))
    q_rot = low(rotate(normalize(q_raw) * q_gain, cosine_tab, sine_tab, 1.0))
    k_rot = low(rotate(normalize(k_raw) * k_gain, cosine_tab, sine_tab, 1.0))
    v_low = low(v_raw)
    scores = low_back(jnp.einsum('qhe,khe->hqk', q_rot, k_rot, precision=HIGHEST_PREC) * HD ** (-0.5))
    allowed = (doc_id[:, None] == doc_id[None, :]) & (token_index[None, :] <= token_index[:, None])
    attn_probs = low(jax.nn.softmax(jnp.where(allowed[None], scores, MASKED), axis=-1))
    attended = jnp.einsum('hqk,khe->qhe', attn_probs, v_low, precision=HIGHEST_PREC).reshape(TOK_DEV, HQ * HD)
    attended = low(low_back(attended))
    hidden_state = x_seq + low_back(jnp.dot(attended, w_out, precision=HIGHEST_PREC))
    xn_two = low(normalize(hidden_state) * gain_two)
    gate_act = low_back(jnp.dot(xn_two, w_gate, precision=HIGHEST_PREC))
    up_act = low_back(jnp.dot(xn_two, w_up, precision=HIGHEST_PREC))
    ffn_hidden = low(jax.nn.silu(gate_act) * up_act * live_cols)
    return hidden_state + low_back(jnp.dot(ffn_hidden, w_down, precision=HIGHEST_PREC))

def forward(x_all, gain_one, w_query, w_keyval, q_gain, k_gain, w_out, gain_two, w_gate, w_up, w_down, doc_lengths, live_cols):
    step_fn = jax.checkpoint(sequence)

    def one_row(carry, item):
        return (carry, step_fn(item[0], item[1], live_cols, gain_one, w_query, w_keyval, q_gain, k_gain, w_out, gain_two, w_gate, w_up, w_down))
    _, outputs = lax.scan(one_row, jnp.zeros((), jnp.float32), (x_all.reshape(N_DP, TOK_DEV, D), doc_lengths))
    return outputs.reshape(N_DP * TOK_DEV, D)

def reference(tokens, doc_lengths, slot_live, attn_gain, w_query, w_keyval, q_gain, k_gain, w_out, ffn_gain, w_gate, w_up, w_down, out_grad):
    live_cols = jnp.repeat(slot_live.astype(jnp.float32), TILE)
    floats = tuple((a.astype(jnp.float32) for a in (tokens, attn_gain, w_query, w_keyval, q_gain, k_gain, w_out, ffn_gain, w_gate, w_up, w_down)))

    def wrapped(*params):
        return forward(*params, doc_lengths, live_cols)
    result, pullback = jax.vjp(wrapped, *floats)
    grads = pullback(out_grad.astype(jnp.float32))
    return (result.astype(jnp.bfloat16), grads[0], grads[1], grads[2], grads[3], grads[4], grads[5], grads[6], grads[7], grads[8], grads[9], grads[10])
```

```python
import math

import jax
import jax.numpy as jnp
from jax import lax
from jax.sharding import PartitionSpec as P

EPSILON = 1e-06
MASKED = -1000000000.0
ROPE_BASE = 10000.0
HIGHEST_PREC = lax.Precision.HIGHEST
CONTRACT_LAST = (((1,), (1,)), ((), ()))
CONTRACT_FIRST = (((0,), (0,)), ((), ()))


def normalize(raw_in):
    return raw_in * lax.rsqrt(jnp.mean(raw_in * raw_in, axis=-1, keepdims=True) + EPSILON)


def norm_back(grad_normed, raw_in, gain_vec):
    factor = lax.rsqrt(jnp.mean(raw_in * raw_in, axis=-1, keepdims=True) + EPSILON)
    unit_rows = raw_in * factor
    scaled = grad_normed * gain_vec
    grad_raw = factor * (scaled - unit_rows * jnp.mean(scaled * unit_rows, axis=-1, keepdims=True))
    return (grad_raw, jnp.sum(grad_normed * unit_rows, axis=tuple(range(raw_in.ndim - 1))))


def rotate(values, cosine_tab, sine_tab, sign):
    half_size = values.shape[-1] // 2
    first_half = values[..., :half_size]
    second_half = values[..., half_size:]
    return jnp.concatenate(
        [
            first_half * cosine_tab - sign * second_half * sine_tab,
            second_half * cosine_tab + sign * first_half * sine_tab,
        ],
        axis=-1,
    )


def doc_layout(lengths, row_count):
    doc_ends = jnp.cumsum(lengths)
    token_index = jnp.arange(row_count, dtype=jnp.int32)
    past_end = (token_index[:, None] >= doc_ends[None, :]).astype(jnp.int32)
    doc_id = jnp.sum(past_end, axis=1)
    doc_pos = token_index - jnp.sum(past_end * lengths[None, :], axis=1)
    return (doc_id, doc_pos, token_index)


def rope_table(doc_pos, head_size):
    rope_freq = jnp.exp(
        jnp.arange(head_size // 2, dtype=jnp.float32) * (-2.0 * math.log(ROPE_BASE) / head_size)
    )
    rope_angle = doc_pos.astype(jnp.float32)[:, None] * rope_freq[None, :]
    return (jnp.cos(rope_angle)[:, None, :], jnp.sin(rope_angle)[:, None, :])


def shards(
    tokens,
    doc_lengths,
    slot_live,
    attn_gain,
    w_query,
    w_keyval,
    q_gain,
    k_gain,
    w_out,
    ffn_gain,
    w_gate,
    w_up,
    w_down,
    out_grad,
):
    row_count, model_width = tokens.shape
    head_size = q_gain.shape[0]
    heads_dev = w_query.shape[1] // head_size
    heads_all = heads_dev * lax.axis_size("mp")
    kv_heads = w_keyval.shape[1] // (2 * head_size)
    group_size = heads_all // kv_heads
    kv_window = min(kv_heads, (heads_dev + group_size - 2) // group_size + 1)
    tile_cols = w_gate.shape[1] // slot_live.shape[0]
    shard_rows = row_count // lax.axis_size("mp")
    block_rows = min(512, row_count)
    score_scale = head_size ** (-0.5)
    head_span = heads_dev * head_size
    mp_index = lax.axis_index("mp")
    row_first = mp_index * shard_rows
    q_first = mp_index * heads_dev
    kv_first = jnp.minimum(q_first // group_size, kv_heads - kv_window)
    kv_owner = (q_first + jnp.arange(heads_dev, dtype=jnp.int32)) // group_size - kv_first
    head_pick = (kv_owner[:, None] == jnp.arange(kv_window, dtype=jnp.int32)[None, :]).astype(
        jnp.float32
    )
    key_cols = lax.dynamic_slice_in_dim(w_keyval, kv_first * head_size, kv_window * head_size, 1)
    value_cols = lax.dynamic_slice_in_dim(
        w_keyval, (kv_heads + kv_first) * head_size, kv_window * head_size, 1
    )

    def spread(window_cols):
        return (
            jnp.einsum(
                "dwe,hw->dhe",
                window_cols.reshape(model_width, kv_window, head_size),
                head_pick.astype(jnp.bfloat16),
                preferred_element_type=jnp.float32,
            )
            .astype(jnp.bfloat16)
            .reshape(model_width, head_span)
        )

    def fold_heads(per_head):
        return jnp.einsum(
            "dhe,hw->dwe",
            per_head.reshape(model_width, heads_dev, head_size),
            head_pick,
            precision=HIGHEST_PREC,
        ).reshape(model_width, kv_window * head_size)

    doc_id, doc_pos, token_index = doc_layout(doc_lengths[0], row_count)
    cosine_tab, sine_tab = rope_table(doc_pos, head_size)
    x_float = tokens.astype(jnp.float32)
    x_rows = lax.dynamic_slice_in_dim(x_float, row_first, shard_rows, 0)
    gain_one = attn_gain.astype(jnp.float32)
    gain_two = ffn_gain.astype(jnp.float32)
    q_gain_f = q_gain.astype(jnp.float32)
    k_gain_f = k_gain.astype(jnp.float32)
    xn_one = (normalize(x_float) * gain_one).astype(jnp.bfloat16)
    q_raw = jnp.dot(xn_one, w_query, preferred_element_type=jnp.float32).reshape(
        row_count, heads_dev, head_size
    )
    kv_raw = jnp.dot(
        xn_one, jnp.concatenate([key_cols, value_cols], axis=1), preferred_element_type=jnp.float32
    ).reshape(row_count, 2, kv_window, head_size)
    k_raw = jnp.einsum("twe,hw->the", kv_raw[:, 0], head_pick, precision=HIGHEST_PREC)
    v_raw = jnp.einsum("twe,hw->the", kv_raw[:, 1], head_pick, precision=HIGHEST_PREC)
    q_rot = rotate(normalize(q_raw) * q_gain_f, cosine_tab, sine_tab, 1.0).astype(jnp.bfloat16)
    k_rot = rotate(normalize(k_raw) * k_gain_f, cosine_tab, sine_tab, 1.0).astype(jnp.bfloat16)
    v_low = v_raw.astype(jnp.bfloat16)

    def block_scores(row_start, key_stop):
        scores = (
            jnp.einsum(
                "qhe,khe->hqk",
                q_rot[row_start : row_start + block_rows],
                k_rot[:key_stop],
                preferred_element_type=jnp.float32,
            )
            * score_scale
        )
        allowed = (doc_id[row_start : row_start + block_rows, None] == doc_id[None, :key_stop]) & (
            token_index[None, :key_stop] <= token_index[row_start : row_start + block_rows, None]
        )
        return jnp.where(allowed[None], scores, MASKED)

    block_outs = []
    block_lse = []
    for row_start in range(0, row_count, block_rows):
        key_stop = row_start + block_rows
        scores = block_scores(row_start, key_stop)
        row_max = jnp.max(scores, axis=-1, keepdims=True)
        shifted = jnp.exp(scores - row_max)
        row_total = jnp.sum(shifted, axis=-1, keepdims=True)
        attn_probs = (shifted / row_total).astype(jnp.bfloat16)
        block_outs.append(
            jnp.einsum(
                "hqk,khe->qhe", attn_probs, v_low[:key_stop], preferred_element_type=jnp.float32
            )
        )
        block_lse.append(row_max + jnp.log(row_total))
    attended = (
        jnp.concatenate(block_outs, axis=0).reshape(row_count, head_span).astype(jnp.bfloat16)
    )
    attn_part = jnp.dot(attended, w_out, preferred_element_type=jnp.float32)
    hidden_rows = x_rows + lax.psum_scatter(
        attn_part.astype(jnp.bfloat16), "mp", scatter_dimension=0, tiled=True
    ).astype(jnp.float32)
    xn_two = lax.all_gather(
        (normalize(hidden_rows) * gain_two).astype(jnp.bfloat16), "mp", axis=0, tiled=True
    )
    live_cols = jnp.repeat(slot_live.astype(jnp.float32), tile_cols)
    gate_act = jnp.dot(xn_two, w_gate, preferred_element_type=jnp.float32)
    up_act = jnp.dot(xn_two, w_up, preferred_element_type=jnp.float32)
    gate_sigmoid = jax.nn.sigmoid(gate_act)
    gate_silu = gate_act * gate_sigmoid
    ffn_hidden = (gate_silu * up_act * live_cols).astype(jnp.bfloat16)
    ffn_part = jnp.dot(ffn_hidden, w_down, preferred_element_type=jnp.float32)
    out_rows = hidden_rows + lax.psum_scatter(
        ffn_part.astype(jnp.bfloat16), "mp", scatter_dimension=0, tiled=True
    ).astype(jnp.float32)
    block_out = out_rows.astype(jnp.bfloat16)
    d_hidden = (
        lax.dot_general(out_grad, w_down, CONTRACT_LAST, preferred_element_type=jnp.float32)
        * live_cols
    )
    grad_down = lax.dot_general(
        ffn_hidden, out_grad, CONTRACT_FIRST, preferred_element_type=jnp.float32
    )
    d_gate = (d_hidden * up_act * gate_sigmoid * (1.0 + gate_act * (1.0 - gate_sigmoid))).astype(
        jnp.bfloat16
    )
    d_up = (d_hidden * gate_silu).astype(jnp.bfloat16)
    grad_gate = lax.dot_general(xn_two, d_gate, CONTRACT_FIRST, preferred_element_type=jnp.float32)
    grad_up = lax.dot_general(xn_two, d_up, CONTRACT_FIRST, preferred_element_type=jnp.float32)
    dn_two_part = lax.dot_general(
        d_gate, w_gate, CONTRACT_LAST, preferred_element_type=jnp.float32
    ) + lax.dot_general(d_up, w_up, CONTRACT_LAST, preferred_element_type=jnp.float32)
    dn_two_rows = lax.psum_scatter(
        dn_two_part.astype(jnp.bfloat16), "mp", scatter_dimension=0, tiled=True
    ).astype(jnp.float32)
    back_two, grad_gain_two = norm_back(dn_two_rows, hidden_rows, gain_two)
    g_rows = lax.dynamic_slice_in_dim(out_grad, row_first, shard_rows, 0)
    dh_rows = g_rows.astype(jnp.float32) + back_two
    dh_low = lax.all_gather(dh_rows.astype(jnp.bfloat16), "mp", axis=0, tiled=True)
    grad_out_proj = lax.dot_general(
        attended, dh_low, CONTRACT_FIRST, preferred_element_type=jnp.float32
    )
    d_att = lax.dot_general(dh_low, w_out, CONTRACT_LAST, preferred_element_type=jnp.float32)
    d_att = d_att.astype(jnp.bfloat16).reshape(row_count, heads_dev, head_size)
    dq_blocks = []
    d_keys = jnp.zeros((row_count, heads_dev, head_size), jnp.float32)
    d_values = jnp.zeros((row_count, heads_dev, head_size), jnp.float32)
    for block_index, row_start in enumerate(range(0, row_count, block_rows)):
        key_stop = row_start + block_rows
        scores = block_scores(row_start, key_stop)
        attn_probs = jnp.exp(scores - block_lse[block_index])
        probs_low = attn_probs.astype(jnp.bfloat16)
        att_rows = d_att[row_start:key_stop]
        d_probs = jnp.einsum(
            "qhe,khe->hqk", att_rows, v_low[:key_stop], preferred_element_type=jnp.float32
        )
        d_scores = (
            attn_probs * (d_probs - jnp.sum(d_probs * attn_probs, axis=-1, keepdims=True))
        ).astype(jnp.bfloat16)
        dq_blocks.append(
            jnp.einsum(
                "hqk,khe->qhe", d_scores, k_rot[:key_stop], preferred_element_type=jnp.float32
            )
            * score_scale
        )
        d_keys = d_keys.at[:key_stop].add(
            jnp.einsum(
                "hqk,qhe->khe",
                d_scores,
                q_rot[row_start:key_stop],
                preferred_element_type=jnp.float32,
            )
            * score_scale
        )
        d_values = d_values.at[:key_stop].add(
            jnp.einsum("hqk,qhe->khe", probs_low, att_rows, preferred_element_type=jnp.float32)
        )
    d_queries = jnp.concatenate(dq_blocks, axis=0)
    dq_raw, grad_q_gain = norm_back(rotate(d_queries, cosine_tab, sine_tab, -1.0), q_raw, q_gain_f)
    dk_raw, grad_k_gain = norm_back(rotate(d_keys, cosine_tab, sine_tab, -1.0), k_raw, k_gain_f)
    d_proj = jnp.concatenate(
        [
            dq_raw.reshape(row_count, head_span),
            dk_raw.reshape(row_count, head_span),
            d_values.reshape(row_count, head_span),
        ],
        axis=1,
    ).astype(jnp.bfloat16)
    w_proj = jnp.concatenate([w_query, spread(key_cols), spread(value_cols)], axis=1)
    dn_one_part = lax.dot_general(d_proj, w_proj, CONTRACT_LAST, preferred_element_type=jnp.float32)
    grad_proj = lax.dot_general(xn_one, d_proj, CONTRACT_FIRST, preferred_element_type=jnp.float32)
    grad_query = grad_proj[:, :head_span]
    keyval_window = jnp.concatenate(
        [
            fold_heads(grad_proj[:, head_span : 2 * head_span]),
            fold_heads(grad_proj[:, 2 * head_span :]),
        ],
        axis=1,
    ).astype(jnp.bfloat16)
    keyval_rows = lax.psum_scatter(keyval_window, "dp", scatter_dimension=0, tiled=True)
    window_span = kv_window * head_size
    grad_keyval = jnp.zeros((keyval_rows.shape[0], 2 * kv_heads * head_size), jnp.bfloat16)
    grad_keyval = lax.dynamic_update_slice_in_dim(
        grad_keyval, keyval_rows[:, :window_span], kv_first * head_size, 1
    )
    grad_keyval = lax.dynamic_update_slice_in_dim(
        grad_keyval, keyval_rows[:, window_span:], (kv_heads + kv_first) * head_size, 1
    )
    grad_keyval = lax.psum_scatter(grad_keyval, "mp", scatter_dimension=0, tiled=True).astype(
        jnp.float32
    )
    dn_one_rows = lax.psum_scatter(
        dn_one_part.astype(jnp.bfloat16), "mp", scatter_dimension=0, tiled=True
    ).astype(jnp.float32)
    back_one, grad_gain_one = norm_back(dn_one_rows, x_rows, gain_one)
    grad_tokens = dh_rows + back_one
    grad_query, grad_out_proj, grad_gate, grad_up, grad_down = (
        lax.psum_scatter(
            grad_query.astype(jnp.bfloat16), "dp", scatter_dimension=0, tiled=True
        ).astype(jnp.float32),
        lax.psum_scatter(
            grad_out_proj.astype(jnp.bfloat16), "dp", scatter_dimension=1, tiled=True
        ).astype(jnp.float32),
        lax.psum_scatter(
            grad_gate.astype(jnp.bfloat16), "dp", scatter_dimension=0, tiled=True
        ).astype(jnp.float32),
        lax.psum_scatter(
            grad_up.astype(jnp.bfloat16), "dp", scatter_dimension=0, tiled=True
        ).astype(jnp.float32),
        lax.psum_scatter(
            grad_down.astype(jnp.bfloat16), "dp", scatter_dimension=1, tiled=True
        ).astype(jnp.float32),
    )
    grad_gain_one, grad_gain_two, grad_q_gain, grad_k_gain = lax.psum(
        (grad_gain_one, grad_gain_two, grad_q_gain, grad_k_gain), ("dp", "mp")
    )
    return (
        block_out,
        grad_tokens,
        grad_gain_one,
        grad_query,
        grad_keyval,
        grad_q_gain,
        grad_k_gain,
        grad_out_proj,
        grad_gain_two,
        grad_gate,
        grad_up,
        grad_down,
    )


def solution(mesh):
    return jax.shard_map(
        shards,
        mesh=mesh,
        in_specs=(
            P("dp", None),
            P("dp", None),
            P("mp"),
            P(),
            P(None, "mp"),
            P(),
            P(),
            P(),
            P("mp", None),
            P(),
            P(None, "mp"),
            P(None, "mp"),
            P("mp", None),
            P("dp", None),
        ),
        out_specs=(
            P(("dp", "mp"), None),
            P(("dp", "mp"), None),
            P(),
            P("dp", "mp"),
            P(("dp", "mp"), None),
            P(),
            P(),
            P("mp", "dp"),
            P(),
            P("dp", "mp"),
            P("dp", "mp"),
            P("mp", "dp"),
        ),
        check_vma=False,
    )
```

```python
import functools
import math

import jax
import jax.numpy as jnp
from jax import lax
from jax.experimental import pallas as pl
from jax.experimental.pallas import tpu as pltpu
from jax.sharding import PartitionSpec as P

EPSILON = 1e-06
MASKED = -1000000000.0
ROPE_BASE = 10000.0
HIGHEST_PREC = lax.Precision.HIGHEST
MESH_ID = pl.DeviceIdType.MESH
KERNEL_VMEM = 60 * 1024 * 1024
CONTRACT_LAST = (((1,), (1,)), ((), ()))
CONTRACT_FIRST = (((0,), (0,)), ((), ()))


def exchange_kernel(size, data_ref, out_ref, send_sem, recv_sem, local_sem):
    here = lax.axis_index("mp")
    barrier = pltpu.get_barrier_semaphore()
    for step in range(1, size):
        pl.semaphore_signal(
            barrier, inc=1, device_id={"mp": (here + step) % size}, device_id_type=MESH_ID
        )
    pl.semaphore_wait(barrier, size - 1)
    copies = []
    for step in range(1, size):
        there = (here + step) % size
        copy = pltpu.make_async_remote_copy(
            src_ref=data_ref.at[there],
            dst_ref=out_ref.at[here],
            send_sem=send_sem.at[step],
            recv_sem=recv_sem.at[step],
            device_id={"mp": there},
            device_id_type=MESH_ID,
        )
        copy.start()
        copies.append(copy)
    own = pltpu.make_async_copy(data_ref.at[here], out_ref.at[here], local_sem)
    own.start()
    own.wait()
    for copy in copies:
        copy.wait()


def exchange(data, collective_id):
    size = data.shape[0]
    return pl.pallas_call(
        functools.partial(exchange_kernel, size),
        out_shape=jax.ShapeDtypeStruct(data.shape, data.dtype),
        in_specs=[pl.BlockSpec(memory_space=pltpu.VMEM)],
        out_specs=pl.BlockSpec(memory_space=pltpu.VMEM),
        scratch_shapes=[
            pltpu.SemaphoreType.DMA((size,)),
            pltpu.SemaphoreType.DMA((size,)),
            pltpu.SemaphoreType.DMA,
        ],
        compiler_params=pltpu.CompilerParams(collective_id=collective_id, has_side_effects=True),
        cost_estimate=pl.CostEstimate(flops=0, bytes_accessed=data.size * 32, transcendentals=0),
        name=f"exchange_{collective_id}",
    )(data)


def sum_kernel(mp_size, dp_size, data_ref, out_ref, first, second, total, sems):
    mp_here = lax.axis_index("mp")
    dp_here = lax.axis_index("dp")
    barrier = pltpu.get_barrier_semaphore()
    for step in range(1, mp_size):
        pl.semaphore_signal(
            barrier, inc=1, device_id={"mp": (mp_here + step) % mp_size}, device_id_type=MESH_ID
        )
    for step in range(1, dp_size):
        pl.semaphore_signal(
            barrier, inc=1, device_id={"dp": (dp_here + step) % dp_size}, device_id_type=MESH_ID
        )
    pl.semaphore_wait(barrier, mp_size + dp_size - 2)
    copies = []
    for step in range(1, mp_size):
        copy = pltpu.make_async_remote_copy(
            src_ref=data_ref,
            dst_ref=first.at[step],
            send_sem=sems.at[0, step],
            recv_sem=sems.at[1, step],
            device_id={"mp": (mp_here + step) % mp_size},
            device_id_type=MESH_ID,
        )
        copy.start()
        copies.append(copy)
    value = data_ref[...]
    for step in range(1, mp_size):
        copies[step - 1].wait()
        value = value + first[step]
    total[...] = value
    copies = []
    for step in range(1, dp_size):
        copy = pltpu.make_async_remote_copy(
            src_ref=total,
            dst_ref=second.at[step],
            send_sem=sems.at[2, step],
            recv_sem=sems.at[3, step],
            device_id={"dp": (dp_here + step) % dp_size},
            device_id_type=MESH_ID,
        )
        copy.start()
        copies.append(copy)
    second[0] = value
    for copy in copies:
        copy.wait()
    value = jnp.zeros_like(value)
    for source in range(dp_size):
        value = value + second[(dp_here - source + dp_size) % dp_size]
    out_ref[...] = value


def sum_everywhere(data, collective_id):
    mp_size = lax.axis_size("mp")
    dp_size = lax.axis_size("dp")
    return pl.pallas_call(
        functools.partial(sum_kernel, mp_size, dp_size),
        out_shape=jax.ShapeDtypeStruct(data.shape, data.dtype),
        in_specs=[pl.BlockSpec(memory_space=pltpu.VMEM)],
        out_specs=pl.BlockSpec(memory_space=pltpu.VMEM),
        scratch_shapes=[
            pltpu.VMEM((mp_size,) + data.shape, data.dtype),
            pltpu.VMEM((dp_size,) + data.shape, data.dtype),
            pltpu.VMEM(data.shape, data.dtype),
            pltpu.SemaphoreType.DMA((4, max(mp_size, dp_size))),
        ],
        compiler_params=pltpu.CompilerParams(collective_id=collective_id, has_side_effects=True),
        name=f"sum_everywhere_{collective_id}",
    )(data)


def reduce_kernel(size, splits, count, *refs):
    data_refs, out_refs = refs[:count], refs[count : 2 * count]
    recv_refs, sums_refs = refs[2 * count : 3 * count], refs[3 * count : 4 * count]
    send_sem, recv_sem = refs[4 * count :]
    here = lax.axis_index("dp")
    masks = [1 << index for index in range(size.bit_length() - 1)]
    bit_of = {mask: (here // mask) % 2 for mask in masks}

    def relative(offset):
        place = here
        for mask in masks:
            if offset & mask:
                place = place + mask - 2 * mask * bit_of[mask]
        return place

    barrier = pltpu.get_barrier_semaphore()
    for mask in masks:
        pl.semaphore_signal(
            barrier, inc=1, device_id={"dp": relative(mask)}, device_id_type=MESH_ID
        )
    pl.semaphore_wait(barrier, len(masks))

    items = []
    for split in range(splits):
        for index in range(count):
            turn = (len(items)) % max(1, len(masks) - 1)
            order = masks[:1] + masks[1 + turn :] + masks[1 : 1 + turn]
            rows = data_refs[index].shape[1] // splits
            items.append((index, split * rows, rows, order))
    copies = {}

    def start(item, stage, source_of):
        index, first_row, rows, order = items[item]
        mask = order[stage]
        for offset in range(size):
            if offset & mask and not any(offset & done for done in order[:stage]):
                source = source_of(offset)
                copy = pltpu.make_async_remote_copy(
                    src_ref=source,
                    dst_ref=recv_refs[index].at[offset - 1, pl.ds(first_row, rows)],
                    send_sem=send_sem.at[item, offset],
                    recv_sem=recv_sem.at[item, offset],
                    device_id={"dp": relative(mask)},
                    device_id_type=MESH_ID,
                )
                copy.start()
                copies[(item, offset)] = copy

    def received(item, stage):
        index, first_row, rows, order = items[item]
        return [
            offset
            for offset in range(size)
            if offset & order[stage] and not any(offset & done for done in order[:stage])
        ]

    def add_up(item, stage, offset, store):
        index, first_row, rows, order = items[item]
        place = relative(offset)
        step = 16

        def body(turn, carry):
            at = pl.ds(pl.multiple_of(first_row + turn * step, step), step)
            value = data_refs[index][place, at, :].astype(jnp.float32)
            for done in order[:stage]:
                value = value + recv_refs[index][(offset | done) - 1, at, :].astype(jnp.float32)
            store(index, at, value)
            return carry

        lax.fori_loop(0, rows // step, body, 0)

    for item in range(len(items)):
        index, first_row, rows, order = items[item]
        start(
            item,
            0,
            lambda offset: data_refs[index].at[relative(offset), pl.ds(first_row, rows)],
        )
    for stage in range(1, len(masks)):
        for item in range(len(items)):
            index, first_row, rows, order = items[item]
            for offset in received(item, stage - 1):
                copies[(item, offset)].wait_recv()
            for offset in received(item, stage):

                def store(index, at, value, offset=offset):
                    sums_refs[index][offset // 2 - 1, at, :] = value.astype(jnp.bfloat16)

                add_up(item, stage, offset, store)
            start(
                item,
                stage,
                lambda offset: sums_refs[index].at[offset // 2 - 1, pl.ds(first_row, rows)],
            )
    for item in range(len(items)):
        for offset in received(item, len(masks) - 1):
            copies[(item, offset)].wait_recv()

        def store_out(index, at, value):
            out_refs[index][at, :] = value

        add_up(item, len(masks), 0, store_out)
    for copy in copies.values():
        copy.wait_send()


def reduce_rows(arrays, size, collective_id, splits=2):
    rows = arrays[0].shape[0] // size
    widths = [array.shape[1] for array in arrays]
    count = len(arrays)
    items = count * splits
    total = sum(array.size for array in arrays)
    return pl.pallas_call(
        functools.partial(reduce_kernel, size, splits, count),
        out_shape=[jax.ShapeDtypeStruct((rows, width), jnp.float32) for width in widths],
        in_specs=[pl.BlockSpec(memory_space=pltpu.VMEM)] * count,
        out_specs=[pl.BlockSpec(memory_space=pltpu.VMEM)] * count,
        scratch_shapes=[pltpu.VMEM((size - 1, rows, width), jnp.bfloat16) for width in widths]
        + [pltpu.VMEM((size // 2 - 1, rows, width), jnp.bfloat16) for width in widths]
        + [pltpu.SemaphoreType.DMA((items, size)), pltpu.SemaphoreType.DMA((items, size))],
        compiler_params=pltpu.CompilerParams(
            collective_id=collective_id, has_side_effects=True, vmem_limit_bytes=KERNEL_VMEM
        ),
        cost_estimate=pl.CostEstimate(flops=0, bytes_accessed=total * 12, transcendentals=0),
        name=f"reduce_rows_{collective_id}",
    )(*[array.reshape(size, rows, array.shape[1]) for array in arrays])


def normalize(raw_in):
    return raw_in * lax.rsqrt(jnp.mean(raw_in * raw_in, axis=-1, keepdims=True) + EPSILON)


def norm_back(grad_normed, raw_in, gain_vec):
    factor = lax.rsqrt(jnp.mean(raw_in * raw_in, axis=-1, keepdims=True) + EPSILON)
    unit_rows = raw_in * factor
    scaled = grad_normed * gain_vec
    grad_raw = factor * (scaled - unit_rows * jnp.mean(scaled * unit_rows, axis=-1, keepdims=True))
    return (grad_raw, jnp.sum(grad_normed * unit_rows, axis=tuple(range(raw_in.ndim - 1))))


def rotate(values, cosine_tab, sine_tab, sign):
    half_size = values.shape[-1] // 2
    first_half = values[..., :half_size]
    second_half = values[..., half_size:]
    return jnp.concatenate(
        [
            first_half * cosine_tab - sign * second_half * sine_tab,
            second_half * cosine_tab + sign * first_half * sine_tab,
        ],
        axis=-1,
    )


def doc_layout(lengths, row_count):
    doc_ends = jnp.cumsum(lengths)
    token_index = jnp.arange(row_count, dtype=jnp.int32)
    past_end = (token_index[:, None] >= doc_ends[None, :]).astype(jnp.int32)
    doc_id = jnp.sum(past_end, axis=1)
    doc_pos = token_index - jnp.sum(past_end * lengths[None, :], axis=1)
    return (doc_id, doc_pos, token_index)


def rope_table(doc_pos, head_size):
    rope_freq = jnp.exp(
        jnp.arange(head_size // 2, dtype=jnp.float32) * (-2.0 * math.log(ROPE_BASE) / head_size)
    )
    rope_angle = doc_pos.astype(jnp.float32)[:, None] * rope_freq[None, :]
    return (jnp.cos(rope_angle)[:, None, :], jnp.sin(rope_angle)[:, None, :])


def shards(
    tokens,
    doc_lengths,
    slot_live,
    attn_gain,
    w_query,
    w_keyval,
    q_gain,
    k_gain,
    w_out,
    ffn_gain,
    w_gate,
    w_up,
    w_down,
    out_grad,
):
    row_count, model_width = tokens.shape
    head_size = q_gain.shape[0]
    heads_dev = w_query.shape[1] // head_size
    heads_all = heads_dev * lax.axis_size("mp")
    kv_heads = w_keyval.shape[1] // (2 * head_size)
    group_size = heads_all // kv_heads
    mp_size = lax.axis_size("mp")
    dp_size = lax.axis_size("dp")
    kv_window = max(
        ((index + 1) * heads_dev - 1) // group_size - (index * heads_dev) // group_size + 1
        for index in range(mp_size)
    )
    window_firsts = [
        min(index * heads_dev // group_size, kv_heads - kv_window) for index in range(mp_size)
    ]
    tile_cols = w_gate.shape[1] // slot_live.shape[0]
    shard_rows = row_count // lax.axis_size("mp")
    block_rows = min(512, row_count)
    score_scale = head_size ** (-0.5)
    head_span = heads_dev * head_size
    mp_index = lax.axis_index("mp")
    row_first = mp_index * shard_rows
    q_first = mp_index * heads_dev
    kv_first = jnp.minimum(q_first // group_size, kv_heads - kv_window)
    kv_owner = (q_first + jnp.arange(heads_dev, dtype=jnp.int32)) // group_size - kv_first
    head_pick = (kv_owner[:, None] == jnp.arange(kv_window, dtype=jnp.int32)[None, :]).astype(
        jnp.float32
    )
    key_cols = lax.dynamic_slice_in_dim(w_keyval, kv_first * head_size, kv_window * head_size, 1)
    value_cols = lax.dynamic_slice_in_dim(
        w_keyval, (kv_heads + kv_first) * head_size, kv_window * head_size, 1
    )

    def fold_heads(per_head):
        return jnp.einsum(
            "the,hw->twe",
            per_head.astype(jnp.bfloat16),
            head_pick.astype(jnp.bfloat16),
            preferred_element_type=jnp.float32,
        ).reshape(row_count, kv_window * head_size)

    def unfold_windows(per_source):
        sums = [None] * kv_heads
        for index, first in enumerate(window_firsts):
            for place in range(kv_window):
                part = per_source[index][:, place * head_size : (place + 1) * head_size].astype(
                    jnp.float32
                )
                head = first + place
                sums[head] = part if sums[head] is None else sums[head] + part
        return jnp.concatenate(sums, axis=1)

    dp_index = lax.axis_index("dp")
    out_piece = lax.dynamic_slice_in_dim(
        w_out, dp_index * (head_span // dp_size), head_span // dp_size, 0
    )
    query_piece = lax.dynamic_slice_in_dim(
        w_query, dp_index * (model_width // dp_size), model_width // dp_size, 0
    )
    w_out_full = lax.all_gather(out_piece, ("mp", "dp"), axis=0, tiled=True)
    w_query_full = lax.all_gather(query_piece, ("mp", "dp"), axis=0, tiled=True).reshape(
        mp_size, model_width, head_span
    )
    doc_id, doc_pos, token_index = doc_layout(doc_lengths[0], row_count)
    cosine_tab, sine_tab = rope_table(doc_pos, head_size)
    x_float = tokens.astype(jnp.float32)
    x_rows = lax.dynamic_slice_in_dim(x_float, row_first, shard_rows, 0)
    gain_one = attn_gain.astype(jnp.float32)
    gain_two = ffn_gain.astype(jnp.float32)
    q_gain_f = q_gain.astype(jnp.float32)
    k_gain_f = k_gain.astype(jnp.float32)
    xn_one = (normalize(x_float) * gain_one).astype(jnp.bfloat16)
    q_raw = jnp.dot(xn_one, w_query, preferred_element_type=jnp.float32).reshape(
        row_count, heads_dev, head_size
    )
    kv_raw = jnp.dot(
        xn_one, jnp.concatenate([key_cols, value_cols], axis=1), preferred_element_type=jnp.float32
    ).reshape(row_count, 2, kv_window, head_size)
    k_raw = jnp.einsum("twe,hw->the", kv_raw[:, 0], head_pick, precision=HIGHEST_PREC)
    v_raw = jnp.einsum("twe,hw->the", kv_raw[:, 1], head_pick, precision=HIGHEST_PREC)
    q_rot = rotate(normalize(q_raw) * q_gain_f, cosine_tab, sine_tab, 1.0).astype(jnp.bfloat16)
    k_rot = rotate(normalize(k_raw) * k_gain_f, cosine_tab, sine_tab, 1.0).astype(jnp.bfloat16)
    v_low = v_raw.astype(jnp.bfloat16)

    def block_scores(row_start, key_stop):
        scores = (
            jnp.einsum(
                "qhe,khe->hqk",
                q_rot[row_start : row_start + block_rows],
                k_rot[:key_stop],
                preferred_element_type=jnp.float32,
            )
            * score_scale
        )
        allowed = (doc_id[row_start : row_start + block_rows, None] == doc_id[None, :key_stop]) & (
            token_index[None, :key_stop] <= token_index[row_start : row_start + block_rows, None]
        )
        return jnp.where(allowed[None], scores, MASKED)

    block_outs = []
    block_lse = []
    for row_start in range(0, row_count, block_rows):
        key_stop = row_start + block_rows
        scores = block_scores(row_start, key_stop)
        row_max = jnp.max(scores, axis=-1, keepdims=True)
        shifted = jnp.exp(scores - row_max)
        row_total = jnp.sum(shifted, axis=-1, keepdims=True)
        attn_probs = (shifted / row_total).astype(jnp.bfloat16)
        block_outs.append(
            jnp.einsum(
                "hqk,khe->qhe", attn_probs, v_low[:key_stop], preferred_element_type=jnp.float32
            )
        )
        block_lse.append(row_max + jnp.log(row_total))
    attended = (
        jnp.concatenate(block_outs, axis=0).reshape(row_count, head_span).astype(jnp.bfloat16)
    )
    att_rows_all = exchange(attended.reshape(mp_size, shard_rows, head_span), 1)
    att_rows_cat = jnp.concatenate([att_rows_all[i] for i in range(mp_size)], axis=1)
    hidden_rows = x_rows + jnp.dot(att_rows_cat, w_out_full, preferred_element_type=jnp.float32)
    xn_two = lax.all_gather(
        (normalize(hidden_rows) * gain_two).astype(jnp.bfloat16), "mp", axis=0, tiled=True
    )
    live_cols = jnp.repeat(slot_live.astype(jnp.float32), tile_cols)
    gate_act = jnp.dot(xn_two, w_gate, preferred_element_type=jnp.float32)
    up_act = jnp.dot(xn_two, w_up, preferred_element_type=jnp.float32)
    gate_sigmoid = jax.nn.sigmoid(gate_act)
    gate_silu = gate_act * gate_sigmoid
    ffn_hidden = (gate_silu * up_act * live_cols).astype(jnp.bfloat16)
    ffn_part = jnp.dot(ffn_hidden, w_down, preferred_element_type=jnp.float32)
    out_rows = hidden_rows + lax.psum_scatter(
        ffn_part.astype(jnp.bfloat16), "mp", scatter_dimension=0, tiled=True
    ).astype(jnp.float32)
    block_out = out_rows.astype(jnp.bfloat16)
    d_hidden = (
        lax.dot_general(out_grad, w_down, CONTRACT_LAST, preferred_element_type=jnp.float32)
        * live_cols
    )
    grad_down = lax.dot_general(
        out_grad, ffn_hidden, CONTRACT_FIRST, preferred_element_type=jnp.float32
    ).astype(jnp.bfloat16)
    d_gate = (d_hidden * up_act * gate_sigmoid * (1.0 + gate_act * (1.0 - gate_sigmoid))).astype(
        jnp.bfloat16
    )
    d_up = (d_hidden * gate_silu).astype(jnp.bfloat16)
    grad_gate = lax.dot_general(
        xn_two, d_gate, CONTRACT_FIRST, preferred_element_type=jnp.float32
    ).astype(jnp.bfloat16)
    grad_up = lax.dot_general(
        xn_two, d_up, CONTRACT_FIRST, preferred_element_type=jnp.float32
    ).astype(jnp.bfloat16)
    grad_gate, grad_up, grad_down = reduce_rows(
        (grad_gate, grad_up, grad_down), dp_size, 2
    )
    grad_down = grad_down.T
    dn_two_part = lax.dot_general(
        d_gate, w_gate, CONTRACT_LAST, preferred_element_type=jnp.float32
    ) + lax.dot_general(d_up, w_up, CONTRACT_LAST, preferred_element_type=jnp.float32)
    dn_two_rows = lax.psum_scatter(
        dn_two_part.astype(jnp.bfloat16), "mp", scatter_dimension=0, tiled=True
    ).astype(jnp.float32)
    back_two, grad_gain_two = norm_back(dn_two_rows, hidden_rows, gain_two)
    g_rows = lax.dynamic_slice_in_dim(out_grad, row_first, shard_rows, 0)
    dh_rows = g_rows.astype(jnp.float32) + back_two
    dh_low = lax.all_gather(dh_rows.astype(jnp.bfloat16), "mp", axis=0, tiled=True)
    grad_out_proj = lax.dot_general(
        dh_low, attended, CONTRACT_FIRST, preferred_element_type=jnp.float32
    ).astype(jnp.bfloat16)
    d_att_rows = lax.dot_general(
        dh_rows.astype(jnp.bfloat16), w_out_full, CONTRACT_LAST, preferred_element_type=jnp.float32
    ).astype(jnp.bfloat16)
    d_att_blocks = jnp.stack(
        [d_att_rows[:, i * head_span : (i + 1) * head_span] for i in range(mp_size)]
    )
    d_att = exchange(d_att_blocks, 3).reshape(row_count, heads_dev, head_size)
    dq_blocks = []
    d_keys = jnp.zeros((row_count, heads_dev, head_size), jnp.float32)
    d_values = jnp.zeros((row_count, heads_dev, head_size), jnp.float32)
    for block_index, row_start in enumerate(range(0, row_count, block_rows)):
        key_stop = row_start + block_rows
        scores = block_scores(row_start, key_stop)
        attn_probs = jnp.exp(scores - block_lse[block_index])
        probs_low = attn_probs.astype(jnp.bfloat16)
        att_rows = d_att[row_start:key_stop]
        d_probs = jnp.einsum(
            "qhe,khe->hqk", att_rows, v_low[:key_stop], preferred_element_type=jnp.float32
        )
        d_scores = (
            attn_probs * (d_probs - jnp.sum(d_probs * attn_probs, axis=-1, keepdims=True))
        ).astype(jnp.bfloat16)
        dq_blocks.append(
            jnp.einsum(
                "hqk,khe->qhe", d_scores, k_rot[:key_stop], preferred_element_type=jnp.float32
            )
            * score_scale
        )
        d_keys = d_keys.at[:key_stop].add(
            jnp.einsum(
                "hqk,qhe->khe",
                d_scores,
                q_rot[row_start:key_stop],
                preferred_element_type=jnp.float32,
            )
            * score_scale
        )
        d_values = d_values.at[:key_stop].add(
            jnp.einsum("hqk,qhe->khe", probs_low, att_rows, preferred_element_type=jnp.float32)
        )
    d_queries = jnp.concatenate(dq_blocks, axis=0)
    dq_raw, grad_q_gain = norm_back(rotate(d_queries, cosine_tab, sine_tab, -1.0), q_raw, q_gain_f)
    dk_raw, grad_k_gain = norm_back(rotate(d_keys, cosine_tab, sine_tab, -1.0), k_raw, k_gain_f)
    dq_low = dq_raw.reshape(row_count, head_span).astype(jnp.bfloat16)
    d_window = jnp.concatenate([fold_heads(dk_raw), fold_heads(d_values)], axis=1).astype(
        jnp.bfloat16
    )
    window_span = kv_window * head_size
    d_proj = jnp.concatenate([dq_low, d_window], axis=1)
    d_proj_all = exchange(d_proj.reshape(mp_size, shard_rows, head_span + 2 * window_span), 4)
    d_keyval_rows = jnp.concatenate(
        [
            unfold_windows(d_proj_all[:, :, head_span : head_span + window_span]),
            unfold_windows(d_proj_all[:, :, head_span + window_span :]),
        ],
        axis=1,
    ).astype(jnp.bfloat16)
    dn_one_rows = lax.dot_general(
        d_keyval_rows, w_keyval, CONTRACT_LAST, preferred_element_type=jnp.float32
    )
    for index in range(mp_size):
        dn_one_rows = dn_one_rows + lax.dot_general(
            d_proj_all[index, :, :head_span],
            w_query_full[index],
            CONTRACT_LAST,
            preferred_element_type=jnp.float32,
        )
    back_one, grad_gain_one = norm_back(dn_one_rows, x_rows, gain_one)
    grad_tokens = dh_rows + back_one
    grad_query = lax.dot_general(
        xn_one, dq_low, CONTRACT_FIRST, preferred_element_type=jnp.float32
    ).astype(jnp.bfloat16)
    grad_window = lax.dot_general(
        xn_one, d_window, CONTRACT_FIRST, preferred_element_type=jnp.float32
    ).astype(jnp.bfloat16)
    grad_out_proj, grad_query, grad_window = reduce_rows(
        (grad_out_proj, grad_query, grad_window), dp_size, 5
    )
    grad_out_proj = grad_out_proj.T
    window_rows = exchange(
        grad_window.astype(jnp.bfloat16).reshape(mp_size, -1, 2 * window_span), 6
    )
    grad_keyval = jnp.concatenate(
        [
            unfold_windows(window_rows[:, :, :window_span]),
            unfold_windows(window_rows[:, :, window_span:]),
        ],
        axis=1,
    )
    gain_sizes = (model_width, model_width, head_size, head_size)
    gains = jnp.concatenate([grad_gain_one, grad_gain_two, grad_q_gain, grad_k_gain])
    gain_rows = 8 * pl.cdiv(gains.shape[0], 1024)
    gains = jnp.pad(gains, (0, gain_rows * 128 - gains.shape[0])).reshape(gain_rows, 128)
    gains = sum_everywhere(gains, 7).reshape(-1)
    bounds = [sum(gain_sizes[:i]) for i in range(5)]
    grad_gain_one, grad_gain_two, grad_q_gain, grad_k_gain = (
        gains[bounds[i] : bounds[i + 1]] for i in range(4)
    )
    return (
        block_out,
        grad_tokens,
        grad_gain_one,
        grad_query,
        grad_keyval,
        grad_q_gain,
        grad_k_gain,
        grad_out_proj,
        grad_gain_two,
        grad_gate,
        grad_up,
        grad_down,
    )


def solution(mesh):
    return jax.shard_map(
        shards,
        mesh=mesh,
        in_specs=(
            P("dp", None),
            P("dp", None),
            P("mp"),
            P(),
            P(None, "mp"),
            P(),
            P(),
            P(),
            P("mp", None),
            P(),
            P(None, "mp"),
            P(None, "mp"),
            P("mp", None),
            P("dp", None),
        ),
        out_specs=(
            P(("dp", "mp"), None),
            P(("dp", "mp"), None),
            P(),
            P("dp", "mp"),
            P(("dp", "mp"), None),
            P(),
            P(),
            P("mp", "dp"),
            P(),
            P("dp", "mp"),
            P("dp", "mp"),
            P("mp", "dp"),
        ),
        check_vma=False,
    )
```

```python
import functools
import math

import jax
import jax.numpy as jnp
from jax import lax
from jax.experimental import pallas as pl
from jax.experimental.pallas import tpu as pltpu
from jax.sharding import PartitionSpec as P

EPSILON = 1e-06
MASKED = -1000000000.0
ROPE_BASE = 10000.0
HIGHEST_PREC = lax.Precision.HIGHEST
MESH_ID = pl.DeviceIdType.MESH
KERNEL_VMEM = 60 * 1024 * 1024
CONTRACT_LAST = (((1,), (1,)), ((), ()))
CONTRACT_FIRST = (((0,), (0,)), ((), ()))


def exchange_kernel(size, data_ref, out_ref, send_sem, recv_sem, local_sem):
    here = lax.axis_index("mp")
    barrier = pltpu.get_barrier_semaphore()
    for step in range(1, size):
        pl.semaphore_signal(
            barrier, inc=1, device_id={"mp": (here + step) % size}, device_id_type=MESH_ID
        )
    pl.semaphore_wait(barrier, size - 1)
    copies = []
    for step in range(1, size):
        there = (here + step) % size
        copy = pltpu.make_async_remote_copy(
            src_ref=data_ref.at[there],
            dst_ref=out_ref.at[here],
            send_sem=send_sem.at[step],
            recv_sem=recv_sem.at[step],
            device_id={"mp": there},
            device_id_type=MESH_ID,
        )
        copy.start()
        copies.append(copy)
    own = pltpu.make_async_copy(data_ref.at[here], out_ref.at[here], local_sem)
    own.start()
    own.wait()
    for copy in copies:
        copy.wait()


def exchange(data, collective_id):
    size = data.shape[0]
    return pl.pallas_call(
        functools.partial(exchange_kernel, size),
        out_shape=jax.ShapeDtypeStruct(data.shape, data.dtype),
        in_specs=[pl.BlockSpec(memory_space=pltpu.VMEM)],
        out_specs=pl.BlockSpec(memory_space=pltpu.VMEM),
        scratch_shapes=[
            pltpu.SemaphoreType.DMA((size,)),
            pltpu.SemaphoreType.DMA((size,)),
            pltpu.SemaphoreType.DMA,
        ],
        compiler_params=pltpu.CompilerParams(collective_id=collective_id, has_side_effects=True),
        cost_estimate=pl.CostEstimate(flops=0, bytes_accessed=data.size * 32, transcendentals=0),
        name=f"exchange_{collective_id}",
    )(data)


def sum_kernel(mp_size, dp_size, data_ref, out_ref, first, second, total, sems):
    mp_here = lax.axis_index("mp")
    dp_here = lax.axis_index("dp")
    barrier = pltpu.get_barrier_semaphore()
    for step in range(1, mp_size):
        pl.semaphore_signal(
            barrier, inc=1, device_id={"mp": (mp_here + step) % mp_size}, device_id_type=MESH_ID
        )
    for step in range(1, dp_size):
        pl.semaphore_signal(
            barrier, inc=1, device_id={"dp": (dp_here + step) % dp_size}, device_id_type=MESH_ID
        )
    pl.semaphore_wait(barrier, mp_size + dp_size - 2)
    copies = []
    for step in range(1, mp_size):
        copy = pltpu.make_async_remote_copy(
            src_ref=data_ref,
            dst_ref=first.at[step],
            send_sem=sems.at[0, step],
            recv_sem=sems.at[1, step],
            device_id={"mp": (mp_here + step) % mp_size},
            device_id_type=MESH_ID,
        )
        copy.start()
        copies.append(copy)
    value = data_ref[...]
    for step in range(1, mp_size):
        copies[step - 1].wait()
        value = value + first[step]
    total[...] = value
    copies = []
    for step in range(1, dp_size):
        copy = pltpu.make_async_remote_copy(
            src_ref=total,
            dst_ref=second.at[step],
            send_sem=sems.at[2, step],
            recv_sem=sems.at[3, step],
            device_id={"dp": (dp_here + step) % dp_size},
            device_id_type=MESH_ID,
        )
        copy.start()
        copies.append(copy)
    second[0] = value
    for copy in copies:
        copy.wait()
    value = jnp.zeros_like(value)
    for source in range(dp_size):
        value = value + second[(dp_here - source + dp_size) % dp_size]
    out_ref[...] = value


def sum_everywhere(data, collective_id):
    mp_size = lax.axis_size("mp")
    dp_size = lax.axis_size("dp")
    return pl.pallas_call(
        functools.partial(sum_kernel, mp_size, dp_size),
        out_shape=jax.ShapeDtypeStruct(data.shape, data.dtype),
        in_specs=[pl.BlockSpec(memory_space=pltpu.VMEM)],
        out_specs=pl.BlockSpec(memory_space=pltpu.VMEM),
        scratch_shapes=[
            pltpu.VMEM((mp_size,) + data.shape, data.dtype),
            pltpu.VMEM((dp_size,) + data.shape, data.dtype),
            pltpu.VMEM(data.shape, data.dtype),
            pltpu.SemaphoreType.DMA((4, max(mp_size, dp_size))),
        ],
        compiler_params=pltpu.CompilerParams(collective_id=collective_id, has_side_effects=True),
        name=f"sum_everywhere_{collective_id}",
    )(data)


def reduce_kernel(size, splits, count, *refs):
    data_refs, out_refs = refs[:count], refs[count : 2 * count]
    recv_refs, sums_refs = refs[2 * count : 3 * count], refs[3 * count : 4 * count]
    send_sem, recv_sem = refs[4 * count :]
    here = lax.axis_index("dp")
    masks = [1 << index for index in range(size.bit_length() - 1)]
    bit_of = {mask: (here // mask) % 2 for mask in masks}

    def relative(offset):
        place = here
        for mask in masks:
            if offset & mask:
                place = place + mask - 2 * mask * bit_of[mask]
        return place

    barrier = pltpu.get_barrier_semaphore()
    for mask in masks:
        pl.semaphore_signal(
            barrier, inc=1, device_id={"dp": relative(mask)}, device_id_type=MESH_ID
        )
    pl.semaphore_wait(barrier, len(masks))

    items = []
    for split in range(splits):
        for index in range(count):
            turn = (len(items)) % max(1, len(masks) - 1)
            order = masks[:1] + masks[1 + turn :] + masks[1 : 1 + turn]
            rows = data_refs[index].shape[1] // splits
            items.append((index, split * rows, rows, order))
    copies = {}

    def start(item, stage, source_of):
        index, first_row, rows, order = items[item]
        mask = order[stage]
        for offset in range(size):
            if offset & mask and not any(offset & done for done in order[:stage]):
                source = source_of(offset)
                copy = pltpu.make_async_remote_copy(
                    src_ref=source,
                    dst_ref=recv_refs[index].at[offset - 1, pl.ds(first_row, rows)],
                    send_sem=send_sem.at[item, offset],
                    recv_sem=recv_sem.at[item, offset],
                    device_id={"dp": relative(mask)},
                    device_id_type=MESH_ID,
                )
                copy.start()
                copies[(item, offset)] = copy

    def received(item, stage):
        index, first_row, rows, order = items[item]
        return [
            offset
            for offset in range(size)
            if offset & order[stage] and not any(offset & done for done in order[:stage])
        ]

    def add_up(item, stage, offset, store):
        index, first_row, rows, order = items[item]
        place = relative(offset)
        step = 16

        def body(turn, carry):
            at = pl.ds(pl.multiple_of(first_row + turn * step, step), step)
            value = data_refs[index][place, at, :].astype(jnp.float32)
            for done in order[:stage]:
                value = value + recv_refs[index][(offset | done) - 1, at, :].astype(jnp.float32)
            store(index, at, value)
            return carry

        lax.fori_loop(0, rows // step, body, 0)

    for item in range(len(items)):
        index, first_row, rows, order = items[item]
        start(
            item,
            0,
            lambda offset: data_refs[index].at[relative(offset), pl.ds(first_row, rows)],
        )
    for stage in range(1, len(masks)):
        for item in range(len(items)):
            index, first_row, rows, order = items[item]
            for offset in received(item, stage - 1):
                copies[(item, offset)].wait_recv()
            for offset in received(item, stage):

                def store(index, at, value, offset=offset):
                    sums_refs[index][offset // 2 - 1, at, :] = value.astype(jnp.bfloat16)

                add_up(item, stage, offset, store)
            start(
                item,
                stage,
                lambda offset: sums_refs[index].at[offset // 2 - 1, pl.ds(first_row, rows)],
            )
    for item in range(len(items)):
        for offset in received(item, len(masks) - 1):
            copies[(item, offset)].wait_recv()

        def store_out(index, at, value):
            out_refs[index][at, :] = value

        add_up(item, len(masks), 0, store_out)
    for copy in copies.values():
        copy.wait_send()


def reduce_rows(arrays, size, collective_id, splits=2):
    rows = arrays[0].shape[0] // size
    widths = [array.shape[1] for array in arrays]
    count = len(arrays)
    items = count * splits
    total = sum(array.size for array in arrays)
    return pl.pallas_call(
        functools.partial(reduce_kernel, size, splits, count),
        out_shape=[jax.ShapeDtypeStruct((rows, width), jnp.float32) for width in widths],
        in_specs=[pl.BlockSpec(memory_space=pltpu.VMEM)] * count,
        out_specs=[pl.BlockSpec(memory_space=pltpu.VMEM)] * count,
        scratch_shapes=[pltpu.VMEM((size - 1, rows, width), jnp.bfloat16) for width in widths]
        + [pltpu.VMEM((size // 2 - 1, rows, width), jnp.bfloat16) for width in widths]
        + [pltpu.SemaphoreType.DMA((items, size)), pltpu.SemaphoreType.DMA((items, size))],
        compiler_params=pltpu.CompilerParams(
            collective_id=collective_id, has_side_effects=True, vmem_limit_bytes=KERNEL_VMEM
        ),
        cost_estimate=pl.CostEstimate(flops=0, bytes_accessed=total * 12, transcendentals=0),
        name=f"reduce_rows_{collective_id}",
    )(*[array.reshape(size, rows, array.shape[1]) for array in arrays])


def normalize(raw_in):
    return raw_in * lax.rsqrt(jnp.mean(raw_in * raw_in, axis=-1, keepdims=True) + EPSILON)


def norm_back(grad_normed, raw_in, gain_vec):
    factor = lax.rsqrt(jnp.mean(raw_in * raw_in, axis=-1, keepdims=True) + EPSILON)
    unit_rows = raw_in * factor
    scaled = grad_normed * gain_vec
    grad_raw = factor * (scaled - unit_rows * jnp.mean(scaled * unit_rows, axis=-1, keepdims=True))
    return (grad_raw, jnp.sum(grad_normed * unit_rows, axis=tuple(range(raw_in.ndim - 1))))


def rotate(values, cosine_tab, sine_tab, sign):
    half_size = values.shape[-1] // 2
    first_half = values[..., :half_size]
    second_half = values[..., half_size:]
    return jnp.concatenate(
        [
            first_half * cosine_tab - sign * second_half * sine_tab,
            second_half * cosine_tab + sign * first_half * sine_tab,
        ],
        axis=-1,
    )


def doc_layout(lengths, row_count):
    doc_ends = jnp.cumsum(lengths)
    token_index = jnp.arange(row_count, dtype=jnp.int32)
    past_end = (token_index[:, None] >= doc_ends[None, :]).astype(jnp.int32)
    doc_id = jnp.sum(past_end, axis=1)
    doc_pos = token_index - jnp.sum(past_end * lengths[None, :], axis=1)
    return (doc_id, doc_pos, token_index)


def rope_table(doc_pos, head_size):
    rope_freq = jnp.exp(
        jnp.arange(head_size // 2, dtype=jnp.float32) * (-2.0 * math.log(ROPE_BASE) / head_size)
    )
    rope_angle = doc_pos.astype(jnp.float32)[:, None] * rope_freq[None, :]
    return (jnp.cos(rope_angle)[:, None, :], jnp.sin(rope_angle)[:, None, :])


def shards(
    tokens,
    doc_lengths,
    slot_live,
    attn_gain,
    w_query,
    w_keyval,
    q_gain,
    k_gain,
    w_out,
    ffn_gain,
    w_gate,
    w_up,
    w_down,
    out_grad,
):
    row_count, model_width = tokens.shape
    head_size = q_gain.shape[0]
    heads_dev = w_query.shape[1] // head_size
    heads_all = heads_dev * lax.axis_size("mp")
    kv_heads = w_keyval.shape[1] // (2 * head_size)
    group_size = heads_all // kv_heads
    mp_size = lax.axis_size("mp")
    dp_size = lax.axis_size("dp")
    kv_window = max(
        ((index + 1) * heads_dev - 1) // group_size - (index * heads_dev) // group_size + 1
        for index in range(mp_size)
    )
    window_firsts = [
        min(index * heads_dev // group_size, kv_heads - kv_window) for index in range(mp_size)
    ]
    tile_cols = w_gate.shape[1] // slot_live.shape[0]
    shard_rows = row_count // lax.axis_size("mp")
    block_rows = min(512, row_count)
    score_scale = head_size ** (-0.5)
    head_span = heads_dev * head_size
    mp_index = lax.axis_index("mp")
    row_first = mp_index * shard_rows
    q_first = mp_index * heads_dev
    kv_first = jnp.minimum(q_first // group_size, kv_heads - kv_window)
    kv_owner = (q_first + jnp.arange(heads_dev, dtype=jnp.int32)) // group_size - kv_first
    head_pick = (kv_owner[:, None] == jnp.arange(kv_window, dtype=jnp.int32)[None, :]).astype(
        jnp.float32
    )
    key_cols = lax.dynamic_slice_in_dim(w_keyval, kv_first * head_size, kv_window * head_size, 1)
    value_cols = lax.dynamic_slice_in_dim(
        w_keyval, (kv_heads + kv_first) * head_size, kv_window * head_size, 1
    )

    def fold_heads(per_head):
        return jnp.einsum(
            "the,hw->twe",
            per_head.astype(jnp.bfloat16),
            head_pick.astype(jnp.bfloat16),
            preferred_element_type=jnp.float32,
        ).reshape(row_count, kv_window * head_size)

    def unfold_windows(per_source):
        sums = [None] * kv_heads
        for index, first in enumerate(window_firsts):
            for place in range(kv_window):
                part = per_source[index][:, place * head_size : (place + 1) * head_size].astype(
                    jnp.float32
                )
                head = first + place
                sums[head] = part if sums[head] is None else sums[head] + part
        return jnp.concatenate(sums, axis=1)

    dp_index = lax.axis_index("dp")
    out_piece = lax.dynamic_slice_in_dim(
        w_out, dp_index * (head_span // dp_size), head_span // dp_size, 0
    )
    query_piece = lax.dynamic_slice_in_dim(
        w_query, dp_index * (model_width // dp_size), model_width // dp_size, 0
    )
    w_out_full = lax.all_gather(out_piece, ("mp", "dp"), axis=0, tiled=True)
    doc_id, doc_pos, token_index = doc_layout(doc_lengths[0], row_count)
    cosine_tab, sine_tab = rope_table(doc_pos, head_size)
    x_float = tokens.astype(jnp.float32)
    x_rows = lax.dynamic_slice_in_dim(tokens, row_first, shard_rows, 0).astype(jnp.float32)
    gain_one = attn_gain.astype(jnp.float32)
    gain_two = ffn_gain.astype(jnp.float32)
    q_gain_f = q_gain.astype(jnp.float32)
    k_gain_f = k_gain.astype(jnp.float32)
    xn_one = (normalize(x_float) * gain_one).astype(jnp.bfloat16)
    q_raw = jnp.dot(xn_one, w_query, preferred_element_type=jnp.float32).reshape(
        row_count, heads_dev, head_size
    )
    kv_raw = jnp.dot(
        xn_one, jnp.concatenate([key_cols, value_cols], axis=1), preferred_element_type=jnp.float32
    ).reshape(row_count, 2, kv_window, head_size)
    k_raw = jnp.einsum("twe,hw->the", kv_raw[:, 0], head_pick, precision=HIGHEST_PREC)
    v_raw = jnp.einsum("twe,hw->the", kv_raw[:, 1], head_pick, precision=HIGHEST_PREC)
    q_rot = rotate(normalize(q_raw) * q_gain_f, cosine_tab, sine_tab, 1.0).astype(jnp.bfloat16)
    k_rot = rotate(normalize(k_raw) * k_gain_f, cosine_tab, sine_tab, 1.0).astype(jnp.bfloat16)
    v_low = v_raw.astype(jnp.bfloat16)

    def block_scores(row_start, key_stop):
        scores = (
            jnp.einsum(
                "qhe,khe->hqk",
                q_rot[row_start : row_start + block_rows],
                k_rot[:key_stop],
                preferred_element_type=jnp.float32,
            )
            * score_scale
        )
        allowed = (doc_id[row_start : row_start + block_rows, None] == doc_id[None, :key_stop]) & (
            token_index[None, :key_stop] <= token_index[row_start : row_start + block_rows, None]
        )
        return jnp.where(allowed[None], scores, MASKED)

    block_outs = []
    block_lse = []
    for row_start in range(0, row_count, block_rows):
        key_stop = row_start + block_rows
        scores = block_scores(row_start, key_stop)
        row_max = jnp.max(scores, axis=-1, keepdims=True)
        shifted = jnp.exp(scores - row_max)
        row_total = jnp.sum(shifted, axis=-1, keepdims=True)
        attn_probs = (shifted / row_total).astype(jnp.bfloat16)
        block_outs.append(
            jnp.einsum(
                "hqk,khe->qhe", attn_probs, v_low[:key_stop], preferred_element_type=jnp.float32
            )
        )
        block_lse.append(row_max + jnp.log(row_total))
    attended = (
        jnp.concatenate(block_outs, axis=0).reshape(row_count, head_span).astype(jnp.bfloat16)
    )
    att_rows_all = exchange(attended.reshape(mp_size, shard_rows, head_span), 1)
    att_rows_cat = jnp.concatenate([att_rows_all[i] for i in range(mp_size)], axis=1)
    hidden_rows = x_rows + jnp.dot(att_rows_cat, w_out_full, preferred_element_type=jnp.float32)
    chunks = 2
    chunk_rows = shard_rows // chunks
    xn_two_rows = (normalize(hidden_rows) * gain_two).astype(jnp.bfloat16)
    grad_chunks = out_grad.reshape(mp_size, chunks, chunk_rows, model_width)
    live_cols = jnp.repeat(slot_live.astype(jnp.float32), tile_cols)
    pieces = []
    for chunk in range(chunks):
        xn_two = lax.all_gather(
            xn_two_rows[chunk * chunk_rows : (chunk + 1) * chunk_rows], "mp", axis=0, tiled=True
        )
        grad_chunk = grad_chunks[:, chunk].reshape(mp_size * chunk_rows, model_width)
        gate_act = jnp.dot(xn_two, w_gate, preferred_element_type=jnp.float32)
        up_act = jnp.dot(xn_two, w_up, preferred_element_type=jnp.float32)
        gate_sigmoid = jax.nn.sigmoid(gate_act)
        gate_silu = gate_act * gate_sigmoid
        ffn_hidden = (gate_silu * up_act * live_cols).astype(jnp.bfloat16)
        d_hidden = (
            lax.dot_general(grad_chunk, w_down, CONTRACT_LAST, preferred_element_type=jnp.float32)
            * live_cols
        )
        d_gate = (
            d_hidden * up_act * gate_sigmoid * (1.0 + gate_act * (1.0 - gate_sigmoid))
        ).astype(jnp.bfloat16)
        d_up = (d_hidden * gate_silu).astype(jnp.bfloat16)
        dn_two_part = lax.dot_general(
            d_gate, w_gate, CONTRACT_LAST, preferred_element_type=jnp.float32
        ) + lax.dot_general(d_up, w_up, CONTRACT_LAST, preferred_element_type=jnp.float32)
        dn_two_chunk = lax.psum_scatter(
            dn_two_part.astype(jnp.bfloat16), "mp", scatter_dimension=0, tiled=True
        )
        pieces.append((xn_two, grad_chunk, ffn_hidden, d_gate, d_up, dn_two_chunk))
    xn_two, grad_cat, ffn_hidden, d_gate, d_up, dn_two_rows = (
        jnp.concatenate(parts, axis=0) for parts in zip(*pieces)
    )
    dn_two_rows = dn_two_rows.astype(jnp.float32)
    back_two, grad_gain_two = norm_back(dn_two_rows, hidden_rows, gain_two)
    g_rows = lax.dynamic_slice_in_dim(out_grad, row_first, shard_rows, 0)
    dh_rows = g_rows.astype(jnp.float32) + back_two
    dh_rows_low = dh_rows.astype(jnp.bfloat16)
    dh_low = lax.all_gather(dh_rows_low, "mp", axis=0, tiled=True)
    query_piece, _ = lax.optimization_barrier((query_piece, dh_rows_low))
    w_query_full = lax.all_gather(query_piece, ("mp", "dp"), axis=0, tiled=True).reshape(
        mp_size, model_width, head_span
    )
    d_att_rows = lax.dot_general(
        dh_rows_low, w_out_full, CONTRACT_LAST, preferred_element_type=jnp.float32
    ).astype(jnp.bfloat16)
    d_att_blocks = jnp.stack(
        [d_att_rows[:, i * head_span : (i + 1) * head_span] for i in range(mp_size)]
    )
    d_att = exchange(d_att_blocks, 3)
    xn_two, grad_cat, _ = lax.optimization_barrier((xn_two, grad_cat, d_att))
    d_att = d_att.reshape(row_count, heads_dev, head_size)
    grad_down = lax.dot_general(
        grad_cat, ffn_hidden, CONTRACT_FIRST, preferred_element_type=jnp.float32
    ).astype(jnp.bfloat16)
    grad_gate = lax.dot_general(
        xn_two, d_gate, CONTRACT_FIRST, preferred_element_type=jnp.float32
    ).astype(jnp.bfloat16)
    grad_up = lax.dot_general(
        xn_two, d_up, CONTRACT_FIRST, preferred_element_type=jnp.float32
    ).astype(jnp.bfloat16)
    grad_gate, grad_up, grad_down = reduce_rows(
        (grad_gate, grad_up, grad_down), dp_size, 2
    )
    grad_down = grad_down.T
    ffn_part = jnp.dot(
        ffn_hidden, w_down, preferred_element_type=jnp.float32
    ).astype(jnp.bfloat16)
    ffn_part = ffn_part.reshape(chunks, mp_size, chunk_rows, model_width).swapaxes(0, 1)
    out_rows = hidden_rows + lax.psum_scatter(
        ffn_part.reshape(row_count, model_width), "mp", scatter_dimension=0, tiled=True
    ).astype(jnp.float32)
    block_out = out_rows.astype(jnp.bfloat16)
    dq_blocks = []
    d_keys = jnp.zeros((row_count, heads_dev, head_size), jnp.float32)
    d_values = jnp.zeros((row_count, heads_dev, head_size), jnp.float32)
    for block_index, row_start in enumerate(range(0, row_count, block_rows)):
        key_stop = row_start + block_rows
        scores = block_scores(row_start, key_stop)
        attn_probs = jnp.exp(scores - block_lse[block_index])
        probs_low = attn_probs.astype(jnp.bfloat16)
        att_rows = d_att[row_start:key_stop]
        d_probs = jnp.einsum(
            "qhe,khe->hqk", att_rows, v_low[:key_stop], preferred_element_type=jnp.float32
        )
        d_scores = (
            attn_probs * (d_probs - jnp.sum(d_probs * attn_probs, axis=-1, keepdims=True))
        ).astype(jnp.bfloat16)
        dq_blocks.append(
            jnp.einsum(
                "hqk,khe->qhe", d_scores, k_rot[:key_stop], preferred_element_type=jnp.float32
            )
            * score_scale
        )
        d_keys = d_keys.at[:key_stop].add(
            jnp.einsum(
                "hqk,qhe->khe",
                d_scores,
                q_rot[row_start:key_stop],
                preferred_element_type=jnp.float32,
            )
            * score_scale
        )
        d_values = d_values.at[:key_stop].add(
            jnp.einsum("hqk,qhe->khe", probs_low, att_rows, preferred_element_type=jnp.float32)
        )
    d_queries = jnp.concatenate(dq_blocks, axis=0)
    dq_raw, grad_q_gain = norm_back(rotate(d_queries, cosine_tab, sine_tab, -1.0), q_raw, q_gain_f)
    dk_raw, grad_k_gain = norm_back(rotate(d_keys, cosine_tab, sine_tab, -1.0), k_raw, k_gain_f)
    dq_low = dq_raw.reshape(row_count, head_span).astype(jnp.bfloat16)
    d_window = jnp.concatenate([fold_heads(dk_raw), fold_heads(d_values)], axis=1).astype(
        jnp.bfloat16
    )
    window_span = kv_window * head_size
    d_proj = jnp.concatenate([dq_low, d_window], axis=1)
    d_proj_all = exchange(d_proj.reshape(mp_size, shard_rows, head_span + 2 * window_span), 4)
    d_keyval_rows = jnp.concatenate(
        [
            unfold_windows(d_proj_all[:, :, head_span : head_span + window_span]),
            unfold_windows(d_proj_all[:, :, head_span + window_span :]),
        ],
        axis=1,
    ).astype(jnp.bfloat16)
    dn_one_rows = lax.dot_general(
        d_keyval_rows, w_keyval, CONTRACT_LAST, preferred_element_type=jnp.float32
    )
    for index in range(mp_size):
        dn_one_rows = dn_one_rows + lax.dot_general(
            d_proj_all[index, :, :head_span],
            w_query_full[index],
            CONTRACT_LAST,
            preferred_element_type=jnp.float32,
        )
    back_one, grad_gain_one = norm_back(dn_one_rows, x_rows, gain_one)
    grad_tokens = dh_rows + back_one
    grad_out_proj = lax.dot_general(
        dh_low, attended, CONTRACT_FIRST, preferred_element_type=jnp.float32
    ).astype(jnp.bfloat16)
    grad_query = lax.dot_general(
        xn_one, dq_low, CONTRACT_FIRST, preferred_element_type=jnp.float32
    ).astype(jnp.bfloat16)
    grad_window = lax.dot_general(
        xn_one, d_window, CONTRACT_FIRST, preferred_element_type=jnp.float32
    ).astype(jnp.bfloat16)
    grad_out_proj, grad_query, grad_window = reduce_rows(
        (grad_out_proj, grad_query, grad_window), dp_size, 5
    )
    grad_out_proj = grad_out_proj.T
    window_rows = exchange(
        grad_window.astype(jnp.bfloat16).reshape(mp_size, -1, 2 * window_span), 6
    )
    grad_keyval = jnp.concatenate(
        [
            unfold_windows(window_rows[:, :, :window_span]),
            unfold_windows(window_rows[:, :, window_span:]),
        ],
        axis=1,
    )
    gain_sizes = (model_width, model_width, head_size, head_size)
    gains = jnp.concatenate([grad_gain_one, grad_gain_two, grad_q_gain, grad_k_gain])
    gain_rows = 8 * pl.cdiv(gains.shape[0], 1024)
    gains = jnp.pad(gains, (0, gain_rows * 128 - gains.shape[0])).reshape(gain_rows, 128)
    gains = sum_everywhere(gains, 7).reshape(-1)
    bounds = [sum(gain_sizes[:i]) for i in range(5)]
    grad_gain_one, grad_gain_two, grad_q_gain, grad_k_gain = (
        gains[bounds[i] : bounds[i + 1]] for i in range(4)
    )
    return (
        block_out,
        grad_tokens,
        grad_gain_one,
        grad_query,
        grad_keyval,
        grad_q_gain,
        grad_k_gain,
        grad_out_proj,
        grad_gain_two,
        grad_gate,
        grad_up,
        grad_down,
    )


def solution(mesh):
    return jax.shard_map(
        shards,
        mesh=mesh,
        in_specs=(
            P("dp", None),
            P("dp", None),
            P("mp"),
            P(),
            P(None, "mp"),
            P(),
            P(),
            P(),
            P("mp", None),
            P(),
            P(None, "mp"),
            P(None, "mp"),
            P("mp", None),
            P("dp", None),
        ),
        out_specs=(
            P(("dp", "mp"), None),
            P(("dp", "mp"), None),
            P(),
            P("dp", "mp"),
            P(("dp", "mp"), None),
            P(),
            P(),
            P("mp", "dp"),
            P(),
            P("dp", "mp"),
            P("dp", "mp"),
            P("mp", "dp"),
        ),
        check_vma=False,
    )
```

```python
import functools
import math

import jax
import jax.numpy as jnp
from jax import lax
from jax.experimental import pallas as pl
from jax.experimental.pallas import tpu as pltpu
from jax.sharding import PartitionSpec as P

EPSILON = 1e-06
MASKED = -1000000000.0
ROPE_BASE = 10000.0
HIGHEST_PREC = lax.Precision.HIGHEST
MESH_ID = pl.DeviceIdType.MESH
KERNEL_VMEM = 60 * 1024 * 1024
CONTRACT_LAST = (((1,), (1,)), ((), ()))
CONTRACT_FIRST = (((0,), (0,)), ((), ()))


def exchange_kernel(size, data_ref, out_ref, send_sem, recv_sem, local_sem):
    here = lax.axis_index("mp")
    barrier = pltpu.get_barrier_semaphore()
    for step in range(1, size):
        pl.semaphore_signal(
            barrier, inc=1, device_id={"mp": (here + step) % size}, device_id_type=MESH_ID
        )
    pl.semaphore_wait(barrier, size - 1)
    copies = []
    for step in range(1, size):
        there = (here + step) % size
        copy = pltpu.make_async_remote_copy(
            src_ref=data_ref.at[there],
            dst_ref=out_ref.at[here],
            send_sem=send_sem.at[step],
            recv_sem=recv_sem.at[step],
            device_id={"mp": there},
            device_id_type=MESH_ID,
        )
        copy.start()
        copies.append(copy)
    own = pltpu.make_async_copy(data_ref.at[here], out_ref.at[here], local_sem)
    own.start()
    own.wait()
    for copy in copies:
        copy.wait()


def exchange(data, collective_id):
    size = data.shape[0]
    return pl.pallas_call(
        functools.partial(exchange_kernel, size),
        out_shape=jax.ShapeDtypeStruct(data.shape, data.dtype),
        in_specs=[pl.BlockSpec(memory_space=pltpu.VMEM)],
        out_specs=pl.BlockSpec(memory_space=pltpu.VMEM),
        scratch_shapes=[
            pltpu.SemaphoreType.DMA((size,)),
            pltpu.SemaphoreType.DMA((size,)),
            pltpu.SemaphoreType.DMA,
        ],
        compiler_params=pltpu.CompilerParams(collective_id=collective_id, has_side_effects=True),
        cost_estimate=pl.CostEstimate(flops=0, bytes_accessed=data.size * 32, transcendentals=0),
        name=f"exchange_{collective_id}",
    )(data)


def sum_kernel(mp_size, dp_size, data_ref, out_ref, first, second, total, sems):
    mp_here = lax.axis_index("mp")
    dp_here = lax.axis_index("dp")
    barrier = pltpu.get_barrier_semaphore()
    for step in range(1, mp_size):
        pl.semaphore_signal(
            barrier, inc=1, device_id={"mp": (mp_here + step) % mp_size}, device_id_type=MESH_ID
        )
    for step in range(1, dp_size):
        pl.semaphore_signal(
            barrier, inc=1, device_id={"dp": (dp_here + step) % dp_size}, device_id_type=MESH_ID
        )
    pl.semaphore_wait(barrier, mp_size + dp_size - 2)
    copies = []
    for step in range(1, mp_size):
        copy = pltpu.make_async_remote_copy(
            src_ref=data_ref,
            dst_ref=first.at[step],
            send_sem=sems.at[0, step],
            recv_sem=sems.at[1, step],
            device_id={"mp": (mp_here + step) % mp_size},
            device_id_type=MESH_ID,
        )
        copy.start()
        copies.append(copy)
    value = data_ref[...]
    for step in range(1, mp_size):
        copies[step - 1].wait()
        value = value + first[step]
    total[...] = value
    copies = []
    for step in range(1, dp_size):
        copy = pltpu.make_async_remote_copy(
            src_ref=total,
            dst_ref=second.at[step],
            send_sem=sems.at[2, step],
            recv_sem=sems.at[3, step],
            device_id={"dp": (dp_here + step) % dp_size},
            device_id_type=MESH_ID,
        )
        copy.start()
        copies.append(copy)
    second[0] = value
    for copy in copies:
        copy.wait()
    value = jnp.zeros_like(value)
    for source in range(dp_size):
        value = value + second[(dp_here - source + dp_size) % dp_size]
    out_ref[...] = value


def sum_everywhere(data, collective_id):
    mp_size = lax.axis_size("mp")
    dp_size = lax.axis_size("dp")
    return pl.pallas_call(
        functools.partial(sum_kernel, mp_size, dp_size),
        out_shape=jax.ShapeDtypeStruct(data.shape, data.dtype),
        in_specs=[pl.BlockSpec(memory_space=pltpu.VMEM)],
        out_specs=pl.BlockSpec(memory_space=pltpu.VMEM),
        scratch_shapes=[
            pltpu.VMEM((mp_size,) + data.shape, data.dtype),
            pltpu.VMEM((dp_size,) + data.shape, data.dtype),
            pltpu.VMEM(data.shape, data.dtype),
            pltpu.SemaphoreType.DMA((4, max(mp_size, dp_size))),
        ],
        compiler_params=pltpu.CompilerParams(collective_id=collective_id, has_side_effects=True),
        name=f"sum_everywhere_{collective_id}",
    )(data)


def reduce_kernel(size, splits, count, lefts, lhs_count, *refs):
    lhs_refs, refs = refs[:lhs_count], refs[lhs_count:]
    rhs_refs, out_refs = refs[:count], refs[count : 2 * count]
    data_refs, refs = refs[2 * count : 3 * count], refs[3 * count :]
    recv_refs, sums_refs = refs[:count], refs[count : 2 * count]
    send_sem, recv_sem = refs[2 * count :]
    here = lax.axis_index("dp")
    masks = [1 << index for index in range(size.bit_length() - 1)]
    bit_of = {mask: (here // mask) % 2 for mask in masks}

    def relative(offset):
        place = here
        for mask in masks:
            if offset & mask:
                place = place + mask - 2 * mask * bit_of[mask]
        return place

    barrier = pltpu.get_barrier_semaphore()
    for mask in masks:
        pl.semaphore_signal(
            barrier, inc=1, device_id={"dp": relative(mask)}, device_id_type=MESH_ID
        )
    pl.semaphore_wait(barrier, len(masks))

    items = []
    for split in range(splits):
        for index in range(count):
            turn = (len(items)) % max(1, len(masks) - 1)
            order = masks[:1] + masks[1 + turn :] + masks[1 : 1 + turn]
            rows = data_refs[index].shape[1] // splits
            items.append((index, split * rows, rows, order))
    copies = {}

    def start(item, stage, source_of, only=None):
        index, first_row, rows, order = items[item]
        mask = order[stage]
        for offset in range(size):
            if only is not None and offset != only:
                continue
            if offset & mask and not any(offset & done for done in order[:stage]):
                source = source_of(offset)
                copy = pltpu.make_async_remote_copy(
                    src_ref=source,
                    dst_ref=recv_refs[index].at[offset - 1, pl.ds(first_row, rows)],
                    send_sem=send_sem.at[item, offset],
                    recv_sem=recv_sem.at[item, offset],
                    device_id={"dp": relative(mask)},
                    device_id_type=MESH_ID,
                )
                copy.start()
                copies[(item, offset)] = copy

    def received(item, stage):
        index, first_row, rows, order = items[item]
        return [
            offset
            for offset in range(size)
            if offset & order[stage] and not any(offset & done for done in order[:stage])
        ]

    def add_up(item, stage, offset, store):
        index, first_row, rows, order = items[item]
        place = relative(offset)
        step = 16

        def body(turn, carry):
            at = pl.ds(pl.multiple_of(first_row + turn * step, step), step)
            value = data_refs[index][place, at, :].astype(jnp.float32)
            for done in order[:stage]:
                value = value + recv_refs[index][(offset | done) - 1, at, :].astype(jnp.float32)
            store(index, at, value)
            return carry

        lax.fori_loop(0, rows // step, body, 0)

    block_rows = data_refs[0].shape[1]

    def multiply(offset, index):
        place = here
        for mask in masks:
            place = place + ((offset // mask) % 2) * (mask - 2 * mask * bit_of[mask])
        columns = pl.ds(pl.multiple_of(place * block_rows, block_rows), block_rows)
        data_refs[index][place] = lax.dot_general(
            lhs_refs[lefts[index]][:, columns],
            rhs_refs[index][...],
            CONTRACT_FIRST,
            preferred_element_type=jnp.float32,
        ).astype(jnp.bfloat16)

    def start_first(offset):
        for item in range(len(items)):
            index, first_row, rows, order = items[item]
            start(
                item,
                0,
                lambda offset: data_refs[index].at[relative(offset), pl.ds(first_row, rows)],
                offset,
            )

    for offset in range(1, size, 2):
        for index in range(count):
            multiply(offset, index)
        if offset > 1:
            start_first(offset - 2)

    def own_block(turn, carry):
        for index in range(count):
            multiply(2 * turn, index)
        return carry

    own_block(0, 0)
    start_first(size - 1)
    lax.fori_loop(1, size // 2, own_block, 0)
    for stage in range(1, len(masks)):
        for item in range(len(items)):
            index, first_row, rows, order = items[item]
            for offset in received(item, stage - 1):
                copies[(item, offset)].wait_recv()
            for offset in received(item, stage):

                def store(index, at, value, offset=offset):
                    sums_refs[index][offset // 2 - 1, at, :] = value.astype(jnp.bfloat16)

                add_up(item, stage, offset, store)
            start(
                item,
                stage,
                lambda offset: sums_refs[index].at[offset // 2 - 1, pl.ds(first_row, rows)],
            )
    for item in range(len(items)):
        for offset in received(item, len(masks) - 1):
            copies[(item, offset)].wait_recv()

        def store_out(index, at, value):
            out_refs[index][at, :] = value

        add_up(item, len(masks), 0, store_out)
    for copy in copies.values():
        copy.wait_send()


def reduce_products(lhs, rhs, lefts, size, collective_id, splits=2):
    depth, model_width = lhs[0].shape
    rows = model_width // size
    widths = [array.shape[1] for array in rhs]
    count = len(rhs)
    items = count * splits
    return pl.pallas_call(
        functools.partial(reduce_kernel, size, splits, count, lefts, len(lhs)),
        out_shape=[jax.ShapeDtypeStruct((rows, width), jnp.float32) for width in widths],
        in_specs=[pl.BlockSpec(memory_space=pltpu.VMEM)] * (len(lhs) + count),
        out_specs=[pl.BlockSpec(memory_space=pltpu.VMEM)] * count,
        scratch_shapes=[pltpu.VMEM((size, rows, width), jnp.bfloat16) for width in widths]
        + [pltpu.VMEM((size - 1, rows, width), jnp.bfloat16) for width in widths]
        + [pltpu.VMEM((size // 2 - 1, rows, width), jnp.bfloat16) for width in widths]
        + [pltpu.SemaphoreType.DMA((items, size)), pltpu.SemaphoreType.DMA((items, size))],
        compiler_params=pltpu.CompilerParams(
            collective_id=collective_id, has_side_effects=True, vmem_limit_bytes=KERNEL_VMEM
        ),
        cost_estimate=pl.CostEstimate(
            flops=2 * depth * model_width * sum(widths),
            bytes_accessed=24 * model_width * sum(widths),
            transcendentals=0,
        ),
        name=f"reduce_products_{collective_id}",
    )(*lhs, *rhs)


def normalize(raw_in):
    return raw_in * lax.rsqrt(jnp.mean(raw_in * raw_in, axis=-1, keepdims=True) + EPSILON)


def norm_back(grad_normed, raw_in, gain_vec):
    factor = lax.rsqrt(jnp.mean(raw_in * raw_in, axis=-1, keepdims=True) + EPSILON)
    unit_rows = raw_in * factor
    scaled = grad_normed * gain_vec
    grad_raw = factor * (scaled - unit_rows * jnp.mean(scaled * unit_rows, axis=-1, keepdims=True))
    return (grad_raw, jnp.sum(grad_normed * unit_rows, axis=tuple(range(raw_in.ndim - 1))))


def rotate(values, cosine_tab, sine_tab, sign):
    half_size = values.shape[-1] // 2
    first_half = values[..., :half_size]
    second_half = values[..., half_size:]
    return jnp.concatenate(
        [
            first_half * cosine_tab - sign * second_half * sine_tab,
            second_half * cosine_tab + sign * first_half * sine_tab,
        ],
        axis=-1,
    )


def doc_layout(lengths, row_count):
    doc_ends = jnp.cumsum(lengths)
    token_index = jnp.arange(row_count, dtype=jnp.int32)
    past_end = (token_index[:, None] >= doc_ends[None, :]).astype(jnp.int32)
    doc_id = jnp.sum(past_end, axis=1)
    doc_pos = token_index - jnp.sum(past_end * lengths[None, :], axis=1)
    return (doc_id, doc_pos, token_index)


def rope_table(doc_pos, head_size):
    rope_freq = jnp.exp(
        jnp.arange(head_size // 2, dtype=jnp.float32) * (-2.0 * math.log(ROPE_BASE) / head_size)
    )
    rope_angle = doc_pos.astype(jnp.float32)[:, None] * rope_freq[None, :]
    return (jnp.cos(rope_angle)[:, None, :], jnp.sin(rope_angle)[:, None, :])


def shards(
    tokens,
    doc_lengths,
    slot_live,
    attn_gain,
    w_query,
    w_keyval,
    q_gain,
    k_gain,
    w_out,
    ffn_gain,
    w_gate,
    w_up,
    w_down,
    out_grad,
):
    row_count, model_width = tokens.shape
    head_size = q_gain.shape[0]
    heads_dev = w_query.shape[1] // head_size
    heads_all = heads_dev * lax.axis_size("mp")
    kv_heads = w_keyval.shape[1] // (2 * head_size)
    group_size = heads_all // kv_heads
    mp_size = lax.axis_size("mp")
    dp_size = lax.axis_size("dp")
    kv_window = max(
        ((index + 1) * heads_dev - 1) // group_size - (index * heads_dev) // group_size + 1
        for index in range(mp_size)
    )
    window_firsts = [
        min(index * heads_dev // group_size, kv_heads - kv_window) for index in range(mp_size)
    ]
    tile_cols = w_gate.shape[1] // slot_live.shape[0]
    shard_rows = row_count // lax.axis_size("mp")
    block_rows = min(512, row_count)
    score_scale = head_size ** (-0.5)
    head_span = heads_dev * head_size
    mp_index = lax.axis_index("mp")
    row_first = mp_index * shard_rows
    q_first = mp_index * heads_dev
    kv_first = jnp.minimum(q_first // group_size, kv_heads - kv_window)
    kv_owner = (q_first + jnp.arange(heads_dev, dtype=jnp.int32)) // group_size - kv_first
    head_pick = (kv_owner[:, None] == jnp.arange(kv_window, dtype=jnp.int32)[None, :]).astype(
        jnp.float32
    )
    key_cols = lax.dynamic_slice_in_dim(w_keyval, kv_first * head_size, kv_window * head_size, 1)
    value_cols = lax.dynamic_slice_in_dim(
        w_keyval, (kv_heads + kv_first) * head_size, kv_window * head_size, 1
    )

    def fold_heads(per_head):
        return jnp.einsum(
            "the,hw->twe",
            per_head.astype(jnp.bfloat16),
            head_pick.astype(jnp.bfloat16),
            preferred_element_type=jnp.float32,
        ).reshape(row_count, kv_window * head_size)

    def unfold_windows(per_source):
        sums = [None] * kv_heads
        for index, first in enumerate(window_firsts):
            for place in range(kv_window):
                part = per_source[index][:, place * head_size : (place + 1) * head_size].astype(
                    jnp.float32
                )
                head = first + place
                sums[head] = part if sums[head] is None else sums[head] + part
        return jnp.concatenate(sums, axis=1)

    dp_index = lax.axis_index("dp")
    out_piece = lax.dynamic_slice_in_dim(
        w_out, dp_index * (head_span // dp_size), head_span // dp_size, 0
    )
    query_piece = lax.dynamic_slice_in_dim(
        w_query, dp_index * (model_width // dp_size), model_width // dp_size, 0
    )
    w_out_full = lax.all_gather(out_piece, ("mp", "dp"), axis=0, tiled=True)
    doc_id, doc_pos, token_index = doc_layout(doc_lengths[0], row_count)
    cosine_tab, sine_tab = rope_table(doc_pos, head_size)
    x_float = tokens.astype(jnp.float32)
    x_rows = lax.dynamic_slice_in_dim(tokens, row_first, shard_rows, 0).astype(jnp.float32)
    gain_one = attn_gain.astype(jnp.float32)
    gain_two = ffn_gain.astype(jnp.float32)
    q_gain_f = q_gain.astype(jnp.float32)
    k_gain_f = k_gain.astype(jnp.float32)
    xn_one = (normalize(x_float) * gain_one).astype(jnp.bfloat16)
    q_raw = jnp.dot(xn_one, w_query, preferred_element_type=jnp.float32).reshape(
        row_count, heads_dev, head_size
    )
    kv_raw = jnp.dot(
        xn_one, jnp.concatenate([key_cols, value_cols], axis=1), preferred_element_type=jnp.float32
    ).reshape(row_count, 2, kv_window, head_size)
    k_raw = jnp.einsum("twe,hw->the", kv_raw[:, 0], head_pick, precision=HIGHEST_PREC)
    v_raw = jnp.einsum("twe,hw->the", kv_raw[:, 1], head_pick, precision=HIGHEST_PREC)
    q_rot = rotate(normalize(q_raw) * q_gain_f, cosine_tab, sine_tab, 1.0).astype(jnp.bfloat16)
    k_rot = rotate(normalize(k_raw) * k_gain_f, cosine_tab, sine_tab, 1.0).astype(jnp.bfloat16)
    v_low = v_raw.astype(jnp.bfloat16)

    def block_scores(row_start, key_stop):
        scores = (
            jnp.einsum(
                "qhe,khe->hqk",
                q_rot[row_start : row_start + block_rows],
                k_rot[:key_stop],
                preferred_element_type=jnp.float32,
            )
            * score_scale
        )
        allowed = (doc_id[row_start : row_start + block_rows, None] == doc_id[None, :key_stop]) & (
            token_index[None, :key_stop] <= token_index[row_start : row_start + block_rows, None]
        )
        return jnp.where(allowed[None], scores, MASKED)

    block_outs = []
    block_lse = []
    for row_start in range(0, row_count, block_rows):
        key_stop = row_start + block_rows
        scores = block_scores(row_start, key_stop)
        row_max = jnp.max(scores, axis=-1, keepdims=True)
        shifted = jnp.exp(scores - row_max)
        row_total = jnp.sum(shifted, axis=-1, keepdims=True)
        attn_probs = (shifted / row_total).astype(jnp.bfloat16)
        block_outs.append(
            jnp.einsum(
                "hqk,khe->qhe", attn_probs, v_low[:key_stop], preferred_element_type=jnp.float32
            )
        )
        block_lse.append(row_max + jnp.log(row_total))
    attended = (
        jnp.concatenate(block_outs, axis=0).reshape(row_count, head_span).astype(jnp.bfloat16)
    )
    att_rows_all = exchange(attended.reshape(mp_size, shard_rows, head_span), 1)
    att_rows_cat = jnp.concatenate([att_rows_all[i] for i in range(mp_size)], axis=1)
    hidden_rows = x_rows + jnp.dot(att_rows_cat, w_out_full, preferred_element_type=jnp.float32)
    chunks = 2
    chunk_rows = shard_rows // chunks
    xn_two_rows = (normalize(hidden_rows) * gain_two).astype(jnp.bfloat16)
    grad_chunks = out_grad.reshape(mp_size, chunks, chunk_rows, model_width)
    live_cols = jnp.repeat(slot_live.astype(jnp.float32), tile_cols)
    pieces = []
    for chunk in range(chunks):
        xn_two = lax.all_gather(
            xn_two_rows[chunk * chunk_rows : (chunk + 1) * chunk_rows], "mp", axis=0, tiled=True
        )
        grad_chunk = grad_chunks[:, chunk].reshape(mp_size * chunk_rows, model_width)
        gate_act = jnp.dot(xn_two, w_gate, preferred_element_type=jnp.float32)
        up_act = jnp.dot(xn_two, w_up, preferred_element_type=jnp.float32)
        gate_sigmoid = jax.nn.sigmoid(gate_act)
        gate_silu = gate_act * gate_sigmoid
        ffn_hidden = (gate_silu * up_act * live_cols).astype(jnp.bfloat16)
        d_hidden = (
            lax.dot_general(grad_chunk, w_down, CONTRACT_LAST, preferred_element_type=jnp.float32)
            * live_cols
        )
        d_gate = (
            d_hidden * up_act * gate_sigmoid * (1.0 + gate_act * (1.0 - gate_sigmoid))
        ).astype(jnp.bfloat16)
        d_up = (d_hidden * gate_silu).astype(jnp.bfloat16)
        dn_two_part = lax.dot_general(
            d_gate, w_gate, CONTRACT_LAST, preferred_element_type=jnp.float32
        ) + lax.dot_general(d_up, w_up, CONTRACT_LAST, preferred_element_type=jnp.float32)
        dn_two_chunk = lax.psum_scatter(
            dn_two_part.astype(jnp.bfloat16), "mp", scatter_dimension=0, tiled=True
        )
        pieces.append((xn_two, grad_chunk, ffn_hidden, d_gate, d_up, dn_two_chunk))
    xn_two, grad_cat, ffn_hidden, d_gate, d_up, dn_two_rows = (
        jnp.concatenate(parts, axis=0) for parts in zip(*pieces)
    )
    grad_gate, grad_up, grad_down = reduce_products(
        (xn_two, grad_cat), (d_gate, d_up, ffn_hidden), (0, 0, 1), dp_size, 2
    )
    grad_down = grad_down.T
    dn_two_rows, grad_up = lax.optimization_barrier((dn_two_rows, grad_up))
    dn_two_rows = dn_two_rows.astype(jnp.float32)
    back_two, grad_gain_two = norm_back(dn_two_rows, hidden_rows, gain_two)
    g_rows = lax.dynamic_slice_in_dim(out_grad, row_first, shard_rows, 0)
    dh_rows = g_rows.astype(jnp.float32) + back_two
    dh_rows_low = dh_rows.astype(jnp.bfloat16)
    dh_low = lax.all_gather(dh_rows_low, "mp", axis=0, tiled=True)
    query_piece, _ = lax.optimization_barrier((query_piece, pieces[-1][-1]))
    w_query_full = lax.all_gather(query_piece, ("mp", "dp"), axis=0, tiled=True).reshape(
        mp_size, model_width, head_span
    )
    d_att_rows = lax.dot_general(
        dh_rows_low, w_out_full, CONTRACT_LAST, preferred_element_type=jnp.float32
    ).astype(jnp.bfloat16)
    d_att_blocks = jnp.stack(
        [d_att_rows[:, i * head_span : (i + 1) * head_span] for i in range(mp_size)]
    )
    d_att = exchange(d_att_blocks, 3)
    d_att = d_att.reshape(row_count, heads_dev, head_size)
    ffn_part = jnp.dot(
        ffn_hidden, w_down, preferred_element_type=jnp.float32
    ).astype(jnp.bfloat16)
    ffn_part = ffn_part.reshape(chunks, mp_size, chunk_rows, model_width).swapaxes(0, 1)
    out_rows = hidden_rows + lax.psum_scatter(
        ffn_part.reshape(row_count, model_width), "mp", scatter_dimension=0, tiled=True
    ).astype(jnp.float32)
    block_out = out_rows.astype(jnp.bfloat16)
    dq_blocks = []
    d_keys = jnp.zeros((row_count, heads_dev, head_size), jnp.float32)
    d_values = jnp.zeros((row_count, heads_dev, head_size), jnp.float32)
    for block_index, row_start in enumerate(range(0, row_count, block_rows)):
        key_stop = row_start + block_rows
        scores = block_scores(row_start, key_stop)
        attn_probs = jnp.exp(scores - block_lse[block_index])
        probs_low = attn_probs.astype(jnp.bfloat16)
        att_rows = d_att[row_start:key_stop]
        d_probs = jnp.einsum(
            "qhe,khe->hqk", att_rows, v_low[:key_stop], preferred_element_type=jnp.float32
        )
        d_scores = (
            attn_probs * (d_probs - jnp.sum(d_probs * attn_probs, axis=-1, keepdims=True))
        ).astype(jnp.bfloat16)
        dq_blocks.append(
            jnp.einsum(
                "hqk,khe->qhe", d_scores, k_rot[:key_stop], preferred_element_type=jnp.float32
            )
            * score_scale
        )
        d_keys = d_keys.at[:key_stop].add(
            jnp.einsum(
                "hqk,qhe->khe",
                d_scores,
                q_rot[row_start:key_stop],
                preferred_element_type=jnp.float32,
            )
            * score_scale
        )
        d_values = d_values.at[:key_stop].add(
            jnp.einsum("hqk,qhe->khe", probs_low, att_rows, preferred_element_type=jnp.float32)
        )
    d_queries = jnp.concatenate(dq_blocks, axis=0)
    dq_raw, grad_q_gain = norm_back(rotate(d_queries, cosine_tab, sine_tab, -1.0), q_raw, q_gain_f)
    dk_raw, grad_k_gain = norm_back(rotate(d_keys, cosine_tab, sine_tab, -1.0), k_raw, k_gain_f)
    dq_low = dq_raw.reshape(row_count, head_span).astype(jnp.bfloat16)
    d_window = jnp.concatenate([fold_heads(dk_raw), fold_heads(d_values)], axis=1).astype(
        jnp.bfloat16
    )
    window_span = kv_window * head_size
    d_proj = jnp.concatenate([dq_low, d_window], axis=1)
    d_proj_all = exchange(d_proj.reshape(mp_size, shard_rows, head_span + 2 * window_span), 4)
    d_keyval_rows = jnp.concatenate(
        [
            unfold_windows(d_proj_all[:, :, head_span : head_span + window_span]),
            unfold_windows(d_proj_all[:, :, head_span + window_span :]),
        ],
        axis=1,
    ).astype(jnp.bfloat16)
    dn_one_rows = lax.dot_general(
        d_keyval_rows, w_keyval, CONTRACT_LAST, preferred_element_type=jnp.float32
    )
    for index in range(mp_size):
        dn_one_rows = dn_one_rows + lax.dot_general(
            d_proj_all[index, :, :head_span],
            w_query_full[index],
            CONTRACT_LAST,
            preferred_element_type=jnp.float32,
        )
    back_one, grad_gain_one = norm_back(dn_one_rows, x_rows, gain_one)
    grad_tokens = dh_rows + back_one
    grad_out_proj, grad_query, grad_window = reduce_products(
        (dh_low, xn_one), (attended, dq_low, d_window), (0, 1, 1), dp_size, 5
    )
    grad_out_proj = grad_out_proj.T
    window_rows = exchange(
        grad_window.astype(jnp.bfloat16).reshape(mp_size, -1, 2 * window_span), 6
    )
    grad_keyval = jnp.concatenate(
        [
            unfold_windows(window_rows[:, :, :window_span]),
            unfold_windows(window_rows[:, :, window_span:]),
        ],
        axis=1,
    )
    gain_sizes = (model_width, model_width, head_size, head_size)
    gains = jnp.concatenate([grad_gain_one, grad_gain_two, grad_q_gain, grad_k_gain])
    gain_rows = 8 * pl.cdiv(gains.shape[0], 1024)
    gains = jnp.pad(gains, (0, gain_rows * 128 - gains.shape[0])).reshape(gain_rows, 128)
    gains = sum_everywhere(gains, 7).reshape(-1)
    bounds = [sum(gain_sizes[:i]) for i in range(5)]
    grad_gain_one, grad_gain_two, grad_q_gain, grad_k_gain = (
        gains[bounds[i] : bounds[i + 1]] for i in range(4)
    )
    return (
        block_out,
        grad_tokens,
        grad_gain_one,
        grad_query,
        grad_keyval,
        grad_q_gain,
        grad_k_gain,
        grad_out_proj,
        grad_gain_two,
        grad_gate,
        grad_up,
        grad_down,
    )


def solution(mesh):
    return jax.shard_map(
        shards,
        mesh=mesh,
        in_specs=(
            P("dp", None),
            P("dp", None),
            P("mp"),
            P(),
            P(None, "mp"),
            P(),
            P(),
            P(),
            P("mp", None),
            P(),
            P(None, "mp"),
            P(None, "mp"),
            P("mp", None),
            P("dp", None),
        ),
        out_specs=(
            P(("dp", "mp"), None),
            P(("dp", "mp"), None),
            P(),
            P("dp", "mp"),
            P(("dp", "mp"), None),
            P(),
            P(),
            P("mp", "dp"),
            P(),
            P("dp", "mp"),
            P("dp", "mp"),
            P("mp", "dp"),
        ),
        check_vma=False,
    )
```

```python
import functools
import math

import jax
import jax.numpy as jnp
from jax import lax
from jax.experimental import pallas as pl
from jax.experimental.pallas import tpu as pltpu
from jax.sharding import PartitionSpec as P

EPSILON = 1e-06
MASKED = -1000000000.0
ROPE_BASE = 10000.0
HIGHEST_PREC = lax.Precision.HIGHEST
MESH_ID = pl.DeviceIdType.MESH
KERNEL_VMEM = 60 * 1024 * 1024
CONTRACT_LAST = (((1,), (1,)), ((), ()))
CONTRACT_FIRST = (((0,), (0,)), ((), ()))


def exchange_kernel(size, data_ref, out_ref, send_sem, recv_sem, local_sem):
    here = lax.axis_index("mp")
    barrier = pltpu.get_barrier_semaphore()
    for step in range(1, size):
        pl.semaphore_signal(
            barrier, inc=1, device_id={"mp": (here + step) % size}, device_id_type=MESH_ID
        )
    pl.semaphore_wait(barrier, size - 1)
    copies = []
    for step in range(1, size):
        there = (here + step) % size
        copy = pltpu.make_async_remote_copy(
            src_ref=data_ref.at[there],
            dst_ref=out_ref.at[here],
            send_sem=send_sem.at[step],
            recv_sem=recv_sem.at[step],
            device_id={"mp": there},
            device_id_type=MESH_ID,
        )
        copy.start()
        copies.append(copy)
    own = pltpu.make_async_copy(data_ref.at[here], out_ref.at[here], local_sem)
    own.start()
    own.wait()
    for copy in copies:
        copy.wait()


def exchange(data, collective_id):
    size = data.shape[0]
    return pl.pallas_call(
        functools.partial(exchange_kernel, size),
        out_shape=jax.ShapeDtypeStruct(data.shape, data.dtype),
        in_specs=[pl.BlockSpec(memory_space=pltpu.VMEM)],
        out_specs=pl.BlockSpec(memory_space=pltpu.VMEM),
        scratch_shapes=[
            pltpu.SemaphoreType.DMA((size,)),
            pltpu.SemaphoreType.DMA((size,)),
            pltpu.SemaphoreType.DMA,
        ],
        compiler_params=pltpu.CompilerParams(collective_id=collective_id, has_side_effects=True),
        cost_estimate=pl.CostEstimate(flops=0, bytes_accessed=data.size * 32, transcendentals=0),
        name=f"exchange_{collective_id}",
    )(data)


def sum_kernel(mp_size, dp_size, data_ref, out_ref, first, second, total, sems):
    mp_here = lax.axis_index("mp")
    dp_here = lax.axis_index("dp")
    barrier = pltpu.get_barrier_semaphore()
    for step in range(1, mp_size):
        pl.semaphore_signal(
            barrier, inc=1, device_id={"mp": (mp_here + step) % mp_size}, device_id_type=MESH_ID
        )
    for step in range(1, dp_size):
        pl.semaphore_signal(
            barrier, inc=1, device_id={"dp": (dp_here + step) % dp_size}, device_id_type=MESH_ID
        )
    pl.semaphore_wait(barrier, mp_size + dp_size - 2)
    copies = []
    for step in range(1, mp_size):
        copy = pltpu.make_async_remote_copy(
            src_ref=data_ref,
            dst_ref=first.at[step],
            send_sem=sems.at[0, step],
            recv_sem=sems.at[1, step],
            device_id={"mp": (mp_here + step) % mp_size},
            device_id_type=MESH_ID,
        )
        copy.start()
        copies.append(copy)
    value = data_ref[...]
    for step in range(1, mp_size):
        copies[step - 1].wait()
        value = value + first[step]
    total[...] = value
    copies = []
    for step in range(1, dp_size):
        copy = pltpu.make_async_remote_copy(
            src_ref=total,
            dst_ref=second.at[step],
            send_sem=sems.at[2, step],
            recv_sem=sems.at[3, step],
            device_id={"dp": (dp_here + step) % dp_size},
            device_id_type=MESH_ID,
        )
        copy.start()
        copies.append(copy)
    second[0] = value
    for copy in copies:
        copy.wait()
    value = jnp.zeros_like(value)
    for source in range(dp_size):
        value = value + second[(dp_here - source + dp_size) % dp_size]
    out_ref[...] = value


def sum_everywhere(data, collective_id):
    mp_size = lax.axis_size("mp")
    dp_size = lax.axis_size("dp")
    return pl.pallas_call(
        functools.partial(sum_kernel, mp_size, dp_size),
        out_shape=jax.ShapeDtypeStruct(data.shape, data.dtype),
        in_specs=[pl.BlockSpec(memory_space=pltpu.VMEM)],
        out_specs=pl.BlockSpec(memory_space=pltpu.VMEM),
        scratch_shapes=[
            pltpu.VMEM((mp_size,) + data.shape, data.dtype),
            pltpu.VMEM((dp_size,) + data.shape, data.dtype),
            pltpu.VMEM(data.shape, data.dtype),
            pltpu.SemaphoreType.DMA((4, max(mp_size, dp_size))),
        ],
        compiler_params=pltpu.CompilerParams(collective_id=collective_id, has_side_effects=True),
        name=f"sum_everywhere_{collective_id}",
    )(data)


def reduce_kernel(size, splits, count, lefts, lhs_count, *refs):
    lhs_refs, refs = refs[:lhs_count], refs[lhs_count:]
    rhs_refs, out_refs = refs[:count], refs[count : 2 * count]
    data_refs, refs = refs[2 * count : 3 * count], refs[3 * count :]
    recv_refs, sums_refs = refs[:count], refs[count : 2 * count]
    send_sem, recv_sem = refs[2 * count :]
    here = lax.axis_index("dp")
    masks = [1 << index for index in range(size.bit_length() - 1)]
    bit_of = {mask: (here // mask) % 2 for mask in masks}

    def relative(offset):
        place = here
        for mask in masks:
            if offset & mask:
                place = place + mask - 2 * mask * bit_of[mask]
        return place

    barrier = pltpu.get_barrier_semaphore()
    for mask in masks:
        pl.semaphore_signal(
            barrier, inc=1, device_id={"dp": relative(mask)}, device_id_type=MESH_ID
        )
    pl.semaphore_wait(barrier, len(masks))

    items = []
    for split in range(splits):
        for index in range(count):
            turn = (len(items)) % max(1, len(masks) - 1)
            order = masks[:1] + masks[1 + turn :] + masks[1 : 1 + turn]
            rows = data_refs[index].shape[1] // splits
            items.append((index, split * rows, rows, order))
    copies = {}

    def start(item, stage, source_of, only=None):
        index, first_row, rows, order = items[item]
        mask = order[stage]
        for offset in range(size):
            if only is not None and offset != only:
                continue
            if offset & mask and not any(offset & done for done in order[:stage]):
                source = source_of(offset)
                copy = pltpu.make_async_remote_copy(
                    src_ref=source,
                    dst_ref=recv_refs[index].at[offset - 1, pl.ds(first_row, rows)],
                    send_sem=send_sem.at[item, offset],
                    recv_sem=recv_sem.at[item, offset],
                    device_id={"dp": relative(mask)},
                    device_id_type=MESH_ID,
                )
                copy.start()
                copies[(item, offset)] = copy

    def received(item, stage):
        index, first_row, rows, order = items[item]
        return [
            offset
            for offset in range(size)
            if offset & order[stage] and not any(offset & done for done in order[:stage])
        ]

    def add_up(item, stage, offset, store):
        index, first_row, rows, order = items[item]
        place = relative(offset)
        step = 16

        def body(turn, carry):
            at = pl.ds(pl.multiple_of(first_row + turn * step, step), step)
            value = data_refs[index][place, at, :].astype(jnp.float32)
            for done in order[:stage]:
                value = value + recv_refs[index][(offset | done) - 1, at, :].astype(jnp.float32)
            store(index, at, value)
            return carry

        lax.fori_loop(0, rows // step, body, 0)

    block_rows = data_refs[0].shape[1]

    def multiply(offset, index):
        place = here
        for mask in masks:
            place = place + ((offset // mask) % 2) * (mask - 2 * mask * bit_of[mask])
        columns = pl.ds(pl.multiple_of(place * block_rows, block_rows), block_rows)
        data_refs[index][place] = lax.dot_general(
            lhs_refs[lefts[index]][:, columns],
            rhs_refs[index][...],
            CONTRACT_FIRST,
            preferred_element_type=jnp.float32,
        ).astype(jnp.bfloat16)

    def start_first(offset):
        for item in range(len(items)):
            index, first_row, rows, order = items[item]
            start(
                item,
                0,
                lambda offset: data_refs[index].at[relative(offset), pl.ds(first_row, rows)],
                offset,
            )

    for offset in range(1, size, 2):
        for index in range(count):
            multiply(offset, index)
        if offset > 1:
            start_first(offset - 2)

    def own_block(turn, carry):
        for index in range(count):
            multiply(2 * turn, index)
        return carry

    own_block(0, 0)
    start_first(size - 1)
    lax.fori_loop(1, size // 2, own_block, 0)
    for stage in range(1, len(masks)):
        for item in range(len(items)):
            index, first_row, rows, order = items[item]
            for offset in received(item, stage - 1):
                copies[(item, offset)].wait_recv()
            for offset in received(item, stage):

                def store(index, at, value, offset=offset):
                    sums_refs[index][offset // 2 - 1, at, :] = value.astype(jnp.bfloat16)

                add_up(item, stage, offset, store)
            start(
                item,
                stage,
                lambda offset: sums_refs[index].at[offset // 2 - 1, pl.ds(first_row, rows)],
            )
    for item in range(len(items)):
        for offset in received(item, len(masks) - 1):
            copies[(item, offset)].wait_recv()

        def store_out(index, at, value):
            out_refs[index][at, :] = value

        add_up(item, len(masks), 0, store_out)
    for copy in copies.values():
        copy.wait_send()


def reduce_products(lhs, rhs, lefts, size, collective_id, splits=2):
    depth, model_width = lhs[0].shape
    rows = model_width // size
    widths = [array.shape[1] for array in rhs]
    count = len(rhs)
    items = count * splits
    return pl.pallas_call(
        functools.partial(reduce_kernel, size, splits, count, lefts, len(lhs)),
        out_shape=[jax.ShapeDtypeStruct((rows, width), jnp.float32) for width in widths],
        in_specs=[pl.BlockSpec(memory_space=pltpu.VMEM)] * (len(lhs) + count),
        out_specs=[pl.BlockSpec(memory_space=pltpu.VMEM)] * count,
        scratch_shapes=[pltpu.VMEM((size, rows, width), jnp.bfloat16) for width in widths]
        + [pltpu.VMEM((size - 1, rows, width), jnp.bfloat16) for width in widths]
        + [pltpu.VMEM((size // 2 - 1, rows, width), jnp.bfloat16) for width in widths]
        + [pltpu.SemaphoreType.DMA((items, size)), pltpu.SemaphoreType.DMA((items, size))],
        compiler_params=pltpu.CompilerParams(
            collective_id=collective_id, has_side_effects=True, vmem_limit_bytes=KERNEL_VMEM
        ),
        cost_estimate=pl.CostEstimate(
            flops=2 * depth * model_width * sum(widths),
            bytes_accessed=24 * model_width * sum(widths),
            transcendentals=0,
        ),
        name=f"reduce_products_{collective_id}",
    )(*lhs, *rhs)


def normalize(raw_in):
    return raw_in * lax.rsqrt(jnp.mean(raw_in * raw_in, axis=-1, keepdims=True) + EPSILON)


def norm_back(grad_normed, raw_in, gain_vec):
    factor = lax.rsqrt(jnp.mean(raw_in * raw_in, axis=-1, keepdims=True) + EPSILON)
    unit_rows = raw_in * factor
    scaled = grad_normed * gain_vec
    grad_raw = factor * (scaled - unit_rows * jnp.mean(scaled * unit_rows, axis=-1, keepdims=True))
    return (grad_raw, jnp.sum(grad_normed * unit_rows, axis=tuple(range(raw_in.ndim - 1))))


def rotate(values, cosine_tab, sine_tab, sign):
    half_size = values.shape[-1] // 2
    first_half = values[..., :half_size]
    second_half = values[..., half_size:]
    return jnp.concatenate(
        [
            first_half * cosine_tab - sign * second_half * sine_tab,
            second_half * cosine_tab + sign * first_half * sine_tab,
        ],
        axis=-1,
    )


def doc_layout(lengths, row_count):
    doc_ends = jnp.cumsum(lengths)
    token_index = jnp.arange(row_count, dtype=jnp.int32)
    past_end = (token_index[:, None] >= doc_ends[None, :]).astype(jnp.int32)
    doc_id = jnp.sum(past_end, axis=1)
    doc_pos = token_index - jnp.sum(past_end * lengths[None, :], axis=1)
    return (doc_id, doc_pos, token_index)


def rope_table(doc_pos, head_size):
    rope_freq = jnp.exp(
        jnp.arange(head_size // 2, dtype=jnp.float32) * (-2.0 * math.log(ROPE_BASE) / head_size)
    )
    rope_angle = doc_pos.astype(jnp.float32)[:, None] * rope_freq[None, :]
    return (jnp.cos(rope_angle)[:, None, :], jnp.sin(rope_angle)[:, None, :])


def shards(
    tokens,
    doc_lengths,
    slot_live,
    attn_gain,
    w_query,
    w_keyval,
    q_gain,
    k_gain,
    w_out,
    ffn_gain,
    w_gate,
    w_up,
    w_down,
    out_grad,
):
    row_count, model_width = tokens.shape
    head_size = q_gain.shape[0]
    heads_dev = w_query.shape[1] // head_size
    heads_all = heads_dev * lax.axis_size("mp")
    kv_heads = w_keyval.shape[1] // (2 * head_size)
    group_size = heads_all // kv_heads
    mp_size = lax.axis_size("mp")
    dp_size = lax.axis_size("dp")
    kv_window = max(
        ((index + 1) * heads_dev - 1) // group_size - (index * heads_dev) // group_size + 1
        for index in range(mp_size)
    )
    window_firsts = [
        min(index * heads_dev // group_size, kv_heads - kv_window) for index in range(mp_size)
    ]
    tile_cols = w_gate.shape[1] // slot_live.shape[0]
    shard_rows = row_count // lax.axis_size("mp")
    block_rows = min(512, row_count)
    score_scale = head_size ** (-0.5)
    head_span = heads_dev * head_size
    mp_index = lax.axis_index("mp")
    row_first = mp_index * shard_rows
    q_first = mp_index * heads_dev
    kv_first = jnp.minimum(q_first // group_size, kv_heads - kv_window)
    kv_owner = (q_first + jnp.arange(heads_dev, dtype=jnp.int32)) // group_size - kv_first
    head_pick = (kv_owner[:, None] == jnp.arange(kv_window, dtype=jnp.int32)[None, :]).astype(
        jnp.float32
    )
    key_cols = lax.dynamic_slice_in_dim(w_keyval, kv_first * head_size, kv_window * head_size, 1)
    value_cols = lax.dynamic_slice_in_dim(
        w_keyval, (kv_heads + kv_first) * head_size, kv_window * head_size, 1
    )

    def fold_heads(per_head):
        return jnp.einsum(
            "the,hw->twe",
            per_head.astype(jnp.bfloat16),
            head_pick.astype(jnp.bfloat16),
            preferred_element_type=jnp.float32,
        ).reshape(row_count, kv_window * head_size)

    def unfold_windows(per_source):
        sums = [None] * kv_heads
        for index, first in enumerate(window_firsts):
            for place in range(kv_window):
                part = per_source[index][:, place * head_size : (place + 1) * head_size].astype(
                    jnp.float32
                )
                head = first + place
                sums[head] = part if sums[head] is None else sums[head] + part
        return jnp.concatenate(sums, axis=1)

    dp_index = lax.axis_index("dp")
    out_piece = lax.dynamic_slice_in_dim(
        w_out, dp_index * (head_span // dp_size), head_span // dp_size, 0
    )
    w_out_full = lax.all_gather(out_piece, ("mp", "dp"), axis=0, tiled=True)
    doc_id, doc_pos, token_index = doc_layout(doc_lengths[0], row_count)
    cosine_tab, sine_tab = rope_table(doc_pos, head_size)
    x_float = tokens.astype(jnp.float32)
    x_rows = lax.dynamic_slice_in_dim(tokens, row_first, shard_rows, 0).astype(jnp.float32)
    gain_one = attn_gain.astype(jnp.float32)
    gain_two = ffn_gain.astype(jnp.float32)
    q_gain_f = q_gain.astype(jnp.float32)
    k_gain_f = k_gain.astype(jnp.float32)
    xn_one = (normalize(x_float) * gain_one).astype(jnp.bfloat16)
    q_raw = jnp.dot(xn_one, w_query, preferred_element_type=jnp.float32).reshape(
        row_count, heads_dev, head_size
    )
    kv_raw = jnp.dot(
        xn_one, jnp.concatenate([key_cols, value_cols], axis=1), preferred_element_type=jnp.float32
    ).reshape(row_count, 2, kv_window, head_size)
    k_raw = jnp.einsum("twe,hw->the", kv_raw[:, 0], head_pick, precision=HIGHEST_PREC)
    v_raw = jnp.einsum("twe,hw->the", kv_raw[:, 1], head_pick, precision=HIGHEST_PREC)
    q_rot = rotate(normalize(q_raw) * q_gain_f, cosine_tab, sine_tab, 1.0).astype(jnp.bfloat16)
    k_rot = rotate(normalize(k_raw) * k_gain_f, cosine_tab, sine_tab, 1.0).astype(jnp.bfloat16)
    v_low = v_raw.astype(jnp.bfloat16)

    def block_scores(row_start, key_stop):
        scores = (
            jnp.einsum(
                "qhe,khe->hqk",
                q_rot[row_start : row_start + block_rows],
                k_rot[:key_stop],
                preferred_element_type=jnp.float32,
            )
            * score_scale
        )
        allowed = (doc_id[row_start : row_start + block_rows, None] == doc_id[None, :key_stop]) & (
            token_index[None, :key_stop] <= token_index[row_start : row_start + block_rows, None]
        )
        return jnp.where(allowed[None], scores, MASKED)

    block_outs = []
    block_lse = []
    for row_start in range(0, row_count, block_rows):
        key_stop = row_start + block_rows
        scores = block_scores(row_start, key_stop)
        row_max = jnp.max(scores, axis=-1, keepdims=True)
        shifted = jnp.exp(scores - row_max)
        row_total = jnp.sum(shifted, axis=-1, keepdims=True)
        attn_probs = (shifted / row_total).astype(jnp.bfloat16)
        block_outs.append(
            jnp.einsum(
                "hqk,khe->qhe", attn_probs, v_low[:key_stop], preferred_element_type=jnp.float32
            )
        )
        block_lse.append(row_max + jnp.log(row_total))
    attended = (
        jnp.concatenate(block_outs, axis=0).reshape(row_count, head_span).astype(jnp.bfloat16)
    )
    att_rows_all = exchange(attended.reshape(mp_size, shard_rows, head_span), 1)
    att_rows_cat = jnp.concatenate([att_rows_all[i] for i in range(mp_size)], axis=1)
    hidden_rows = x_rows + jnp.dot(att_rows_cat, w_out_full, preferred_element_type=jnp.float32)
    chunks = 2
    chunk_rows = shard_rows // chunks
    xn_two_rows = (normalize(hidden_rows) * gain_two).astype(jnp.bfloat16)
    grad_chunks = out_grad.reshape(mp_size, chunks, chunk_rows, model_width)
    live_cols = jnp.repeat(slot_live.astype(jnp.float32), tile_cols)
    pieces = []
    for chunk in range(chunks):
        xn_two = lax.all_gather(
            xn_two_rows[chunk * chunk_rows : (chunk + 1) * chunk_rows], "mp", axis=0, tiled=True
        )
        if chunk:
            xn_two, _ = lax.optimization_barrier((xn_two, dn_two_low))
        grad_chunk = grad_chunks[:, chunk].reshape(mp_size * chunk_rows, model_width)
        gate_act = jnp.dot(xn_two, w_gate, preferred_element_type=jnp.float32)
        up_act = jnp.dot(xn_two, w_up, preferred_element_type=jnp.float32)
        gate_sigmoid = jax.nn.sigmoid(gate_act)
        gate_silu = gate_act * gate_sigmoid
        ffn_hidden = (gate_silu * up_act * live_cols).astype(jnp.bfloat16)
        d_hidden = (
            lax.dot_general(grad_chunk, w_down, CONTRACT_LAST, preferred_element_type=jnp.float32)
            * live_cols
        )
        d_gate = (
            d_hidden * up_act * gate_sigmoid * (1.0 + gate_act * (1.0 - gate_sigmoid))
        ).astype(jnp.bfloat16)
        d_up = (d_hidden * gate_silu).astype(jnp.bfloat16)
        dn_two_part = lax.dot_general(
            d_gate, w_gate, CONTRACT_LAST, preferred_element_type=jnp.float32
        ) + lax.dot_general(d_up, w_up, CONTRACT_LAST, preferred_element_type=jnp.float32)
        dn_two_low = dn_two_part.astype(jnp.bfloat16)
        dn_two_chunk = lax.psum_scatter(dn_two_low, "mp", scatter_dimension=0, tiled=True)
        pieces.append((xn_two, grad_chunk, ffn_hidden, d_gate, d_up, dn_two_chunk))
    xn_two, grad_cat, ffn_hidden, d_gate, d_up, dn_two_rows = (
        jnp.concatenate(parts, axis=0) for parts in zip(*pieces)
    )
    ffn_hidden, _ = lax.optimization_barrier((ffn_hidden, dn_two_low))
    ffn_part = jnp.dot(ffn_hidden, w_down, preferred_element_type=jnp.float32).astype(jnp.bfloat16)
    out_chunks = [
        lax.psum_scatter(part, "mp", scatter_dimension=0, tiled=True)
        for part in jnp.split(ffn_part, chunks, axis=0)
    ]
    xn_two, _ = lax.optimization_barrier((xn_two, ffn_part))
    grad_gate, grad_up, grad_down = reduce_products(
        (xn_two, grad_cat), (d_gate, d_up, ffn_hidden), (0, 0, 1), dp_size, 2
    )
    grad_down = grad_down.T
    dn_two_rows, grad_up = lax.optimization_barrier((dn_two_rows, grad_up))
    dn_two_rows = dn_two_rows.astype(jnp.float32)
    back_two, grad_gain_two = norm_back(dn_two_rows, hidden_rows, gain_two)
    g_rows = lax.dynamic_slice_in_dim(out_grad, row_first, shard_rows, 0)
    dh_rows = g_rows.astype(jnp.float32) + back_two
    dh_rows_low = dh_rows.astype(jnp.bfloat16)
    d_att_rows = lax.dot_general(
        dh_rows_low, w_out_full, CONTRACT_LAST, preferred_element_type=jnp.float32
    ).astype(jnp.bfloat16)
    d_att_blocks = jnp.stack(
        [d_att_rows[:, i * head_span : (i + 1) * head_span] for i in range(mp_size)]
    )
    d_att = exchange(d_att_blocks, 3)
    dh_low, d_att, out_chunks = lax.optimization_barrier((dh_rows_low, d_att, out_chunks))
    dh_low = lax.all_gather(dh_low, "mp", axis=0, tiled=True)
    d_att = d_att.reshape(row_count, heads_dev, head_size)
    dq_blocks = []
    d_keys = jnp.zeros((row_count, heads_dev, head_size), jnp.float32)
    d_values = jnp.zeros((row_count, heads_dev, head_size), jnp.float32)
    for block_index, row_start in enumerate(range(0, row_count, block_rows)):
        key_stop = row_start + block_rows
        scores = block_scores(row_start, key_stop)
        attn_probs = jnp.exp(scores - block_lse[block_index])
        probs_low = attn_probs.astype(jnp.bfloat16)
        att_rows = d_att[row_start:key_stop]
        d_probs = jnp.einsum(
            "qhe,khe->hqk", att_rows, v_low[:key_stop], preferred_element_type=jnp.float32
        )
        d_scores = (
            attn_probs * (d_probs - jnp.sum(d_probs * attn_probs, axis=-1, keepdims=True))
        ).astype(jnp.bfloat16)
        dq_blocks.append(
            jnp.einsum(
                "hqk,khe->qhe", d_scores, k_rot[:key_stop], preferred_element_type=jnp.float32
            )
            * score_scale
        )
        d_keys = d_keys.at[:key_stop].add(
            jnp.einsum(
                "hqk,qhe->khe",
                d_scores,
                q_rot[row_start:key_stop],
                preferred_element_type=jnp.float32,
            )
            * score_scale
        )
        d_values = d_values.at[:key_stop].add(
            jnp.einsum("hqk,qhe->khe", probs_low, att_rows, preferred_element_type=jnp.float32)
        )
    d_queries = jnp.concatenate(dq_blocks, axis=0)
    dq_raw, grad_q_gain = norm_back(rotate(d_queries, cosine_tab, sine_tab, -1.0), q_raw, q_gain_f)
    dk_raw, grad_k_gain = norm_back(rotate(d_keys, cosine_tab, sine_tab, -1.0), k_raw, k_gain_f)
    dq_low = dq_raw.reshape(row_count, head_span).astype(jnp.bfloat16)
    d_window = jnp.concatenate([fold_heads(dk_raw), fold_heads(d_values)], axis=1).astype(
        jnp.bfloat16
    )
    window_span = kv_window * head_size
    dn_one_part = (
        lax.dot_general(dq_low, w_query, CONTRACT_LAST, preferred_element_type=jnp.float32)
        + lax.dot_general(
            d_window,
            jnp.concatenate([key_cols, value_cols], axis=1),
            CONTRACT_LAST,
            preferred_element_type=jnp.float32,
        )
    ).astype(jnp.bfloat16)
    dn_one_rows = lax.psum_scatter(dn_one_part, "mp", scatter_dimension=0, tiled=True).astype(
        jnp.float32
    )
    back_one, grad_gain_one = norm_back(dn_one_rows, x_rows, gain_one)
    grad_tokens = dh_rows + back_one
    xn_one, _ = lax.optimization_barrier((xn_one, dn_one_part))
    grad_out_proj, grad_query, grad_window = reduce_products(
        (dh_low, xn_one), (attended, dq_low, d_window), (0, 1, 1), dp_size, 5
    )
    grad_out_proj = grad_out_proj.T
    window_rows = exchange(
        grad_window.astype(jnp.bfloat16).reshape(mp_size, -1, 2 * window_span), 6
    )
    grad_keyval = jnp.concatenate(
        [
            unfold_windows(window_rows[:, :, :window_span]),
            unfold_windows(window_rows[:, :, window_span:]),
        ],
        axis=1,
    )
    out_rows = hidden_rows + jnp.concatenate(out_chunks, axis=0).astype(jnp.float32)
    block_out = out_rows.astype(jnp.bfloat16)
    gain_sizes = (model_width, model_width, head_size, head_size)
    gains = jnp.concatenate([grad_gain_one, grad_gain_two, grad_q_gain, grad_k_gain])
    gain_rows = 8 * pl.cdiv(gains.shape[0], 1024)
    gains = jnp.pad(gains, (0, gain_rows * 128 - gains.shape[0])).reshape(gain_rows, 128)
    gains = sum_everywhere(gains, 7).reshape(-1)
    bounds = [sum(gain_sizes[:i]) for i in range(5)]
    grad_gain_one, grad_gain_two, grad_q_gain, grad_k_gain = (
        gains[bounds[i] : bounds[i + 1]] for i in range(4)
    )
    return (
        block_out,
        grad_tokens,
        grad_gain_one,
        grad_query,
        grad_keyval,
        grad_q_gain,
        grad_k_gain,
        grad_out_proj,
        grad_gain_two,
        grad_gate,
        grad_up,
        grad_down,
    )


def solution(mesh):
    return jax.shard_map(
        shards,
        mesh=mesh,
        in_specs=(
            P("dp", None),
            P("dp", None),
            P("mp"),
            P(),
            P(None, "mp"),
            P(),
            P(),
            P(),
            P("mp", None),
            P(),
            P(None, "mp"),
            P(None, "mp"),
            P("mp", None),
            P("dp", None),
        ),
        out_specs=(
            P(("dp", "mp"), None),
            P(("dp", "mp"), None),
            P(),
            P("dp", "mp"),
            P(("dp", "mp"), None),
            P(),
            P(),
            P("mp", "dp"),
            P(),
            P("dp", "mp"),
            P("dp", "mp"),
            P("mp", "dp"),
        ),
        check_vma=False,
    )
```

```python
import functools
import math

import jax
import jax.numpy as jnp
from jax import lax
from jax.experimental import pallas as pl
from jax.experimental.pallas import tpu as pltpu
from jax.sharding import PartitionSpec as P

EPSILON = 1e-06
MASKED = -1000000000.0
ROPE_BASE = 10000.0
HIGHEST_PREC = lax.Precision.HIGHEST
MESH_ID = pl.DeviceIdType.MESH
KERNEL_VMEM = 60 * 1024 * 1024
CONTRACT_LAST = (((1,), (1,)), ((), ()))
CONTRACT_FIRST = (((0,), (0,)), ((), ()))


def exchange_kernel(size, data_ref, out_ref, send_sem, recv_sem, local_sem):
    here = lax.axis_index("mp")
    barrier = pltpu.get_barrier_semaphore()
    for step in range(1, size):
        pl.semaphore_signal(
            barrier, inc=1, device_id={"mp": (here + step) % size}, device_id_type=MESH_ID
        )
    pl.semaphore_wait(barrier, size - 1)
    copies = []
    for step in range(1, size):
        there = (here + step) % size
        copy = pltpu.make_async_remote_copy(
            src_ref=data_ref.at[there],
            dst_ref=out_ref.at[here],
            send_sem=send_sem.at[step],
            recv_sem=recv_sem.at[step],
            device_id={"mp": there},
            device_id_type=MESH_ID,
        )
        copy.start()
        copies.append(copy)
    own = pltpu.make_async_copy(data_ref.at[here], out_ref.at[here], local_sem)
    own.start()
    own.wait()
    for copy in copies:
        copy.wait()


def exchange(data, collective_id):
    size = data.shape[0]
    return pl.pallas_call(
        functools.partial(exchange_kernel, size),
        out_shape=jax.ShapeDtypeStruct(data.shape, data.dtype),
        in_specs=[pl.BlockSpec(memory_space=pltpu.VMEM)],
        out_specs=pl.BlockSpec(memory_space=pltpu.VMEM),
        scratch_shapes=[
            pltpu.SemaphoreType.DMA((size,)),
            pltpu.SemaphoreType.DMA((size,)),
            pltpu.SemaphoreType.DMA,
        ],
        compiler_params=pltpu.CompilerParams(collective_id=collective_id, has_side_effects=True),
        cost_estimate=pl.CostEstimate(flops=0, bytes_accessed=data.size * 32, transcendentals=0),
        name=f"exchange_{collective_id}",
    )(data)


def sum_kernel(mp_size, dp_size, data_ref, out_ref, first, second, total, sems):
    mp_here = lax.axis_index("mp")
    dp_here = lax.axis_index("dp")
    barrier = pltpu.get_barrier_semaphore()
    for step in range(1, mp_size):
        pl.semaphore_signal(
            barrier, inc=1, device_id={"mp": (mp_here + step) % mp_size}, device_id_type=MESH_ID
        )
    for step in range(1, dp_size):
        pl.semaphore_signal(
            barrier, inc=1, device_id={"dp": (dp_here + step) % dp_size}, device_id_type=MESH_ID
        )
    pl.semaphore_wait(barrier, mp_size + dp_size - 2)
    copies = []
    for step in range(1, mp_size):
        copy = pltpu.make_async_remote_copy(
            src_ref=data_ref,
            dst_ref=first.at[step],
            send_sem=sems.at[0, step],
            recv_sem=sems.at[1, step],
            device_id={"mp": (mp_here + step) % mp_size},
            device_id_type=MESH_ID,
        )
        copy.start()
        copies.append(copy)
    value = data_ref[...]
    for step in range(1, mp_size):
        copies[step - 1].wait()
        value = value + first[step]
    total[...] = value
    copies = []
    for step in range(1, dp_size):
        copy = pltpu.make_async_remote_copy(
            src_ref=total,
            dst_ref=second.at[step],
            send_sem=sems.at[2, step],
            recv_sem=sems.at[3, step],
            device_id={"dp": (dp_here + step) % dp_size},
            device_id_type=MESH_ID,
        )
        copy.start()
        copies.append(copy)
    second[0] = value
    for copy in copies:
        copy.wait()
    value = jnp.zeros_like(value)
    for source in range(dp_size):
        value = value + second[(dp_here - source + dp_size) % dp_size]
    out_ref[...] = value


def sum_everywhere(data, collective_id):
    mp_size = lax.axis_size("mp")
    dp_size = lax.axis_size("dp")
    return pl.pallas_call(
        functools.partial(sum_kernel, mp_size, dp_size),
        out_shape=jax.ShapeDtypeStruct(data.shape, data.dtype),
        in_specs=[pl.BlockSpec(memory_space=pltpu.VMEM)],
        out_specs=pl.BlockSpec(memory_space=pltpu.VMEM),
        scratch_shapes=[
            pltpu.VMEM((mp_size,) + data.shape, data.dtype),
            pltpu.VMEM((dp_size,) + data.shape, data.dtype),
            pltpu.VMEM(data.shape, data.dtype),
            pltpu.SemaphoreType.DMA((4, max(mp_size, dp_size))),
        ],
        compiler_params=pltpu.CompilerParams(collective_id=collective_id, has_side_effects=True),
        name=f"sum_everywhere_{collective_id}",
    )(data)


def reduce_kernel(size, splits, count, lefts, lhs_count, *refs):
    lhs_refs, refs = refs[:lhs_count], refs[lhs_count:]
    rhs_refs, out_refs = refs[:count], refs[count : 2 * count]
    data_refs, refs = refs[2 * count : 3 * count], refs[3 * count :]
    recv_refs, sums_refs = refs[:count], refs[count : 2 * count]
    send_sem, recv_sem = refs[2 * count :]
    here = lax.axis_index("dp")
    masks = [1 << index for index in range(size.bit_length() - 1)]
    bit_of = {mask: (here // mask) % 2 for mask in masks}

    def relative(offset):
        place = here
        for mask in masks:
            if offset & mask:
                place = place + mask - 2 * mask * bit_of[mask]
        return place

    barrier = pltpu.get_barrier_semaphore()
    for mask in masks:
        pl.semaphore_signal(
            barrier, inc=1, device_id={"dp": relative(mask)}, device_id_type=MESH_ID
        )
    pl.semaphore_wait(barrier, len(masks))

    items = []
    for split in range(splits):
        for index in range(count):
            turn = (len(items)) % max(1, len(masks) - 1)
            order = masks[:1] + masks[1 + turn :] + masks[1 : 1 + turn]
            rows = data_refs[index].shape[1] // splits
            items.append((index, split * rows, rows, order))
    copies = {}

    def start(item, stage, source_of, only=None):
        index, first_row, rows, order = items[item]
        mask = order[stage]
        for offset in range(size):
            if only is not None and offset != only:
                continue
            if offset & mask and not any(offset & done for done in order[:stage]):
                source = source_of(offset)
                copy = pltpu.make_async_remote_copy(
                    src_ref=source,
                    dst_ref=recv_refs[index].at[offset - 1, pl.ds(first_row, rows)],
                    send_sem=send_sem.at[item, offset],
                    recv_sem=recv_sem.at[item, offset],
                    device_id={"dp": relative(mask)},
                    device_id_type=MESH_ID,
                )
                copy.start()
                copies[(item, offset)] = copy

    def received(item, stage):
        index, first_row, rows, order = items[item]
        return [
            offset
            for offset in range(size)
            if offset & order[stage] and not any(offset & done for done in order[:stage])
        ]

    def add_up(item, stage, offset, store):
        index, first_row, rows, order = items[item]
        place = relative(offset)
        step = 16

        def body(turn, carry):
            at = pl.ds(pl.multiple_of(first_row + turn * step, step), step)
            value = data_refs[index][place, at, :].astype(jnp.float32)
            for done in order[:stage]:
                value = value + recv_refs[index][(offset | done) - 1, at, :].astype(jnp.float32)
            store(index, at, value)
            return carry

        lax.fori_loop(0, rows // step, body, 0)

    block_rows = data_refs[0].shape[1]

    def multiply(offset, index):
        place = here
        for mask in masks:
            place = place + ((offset // mask) % 2) * (mask - 2 * mask * bit_of[mask])
        columns = pl.ds(pl.multiple_of(place * block_rows, block_rows), block_rows)
        data_refs[index][place] = lax.dot_general(
            lhs_refs[lefts[index]][:, columns],
            rhs_refs[index][...],
            CONTRACT_FIRST,
            preferred_element_type=jnp.float32,
        ).astype(jnp.bfloat16)

    def start_first(offset):
        for item in range(len(items)):
            index, first_row, rows, order = items[item]
            start(
                item,
                0,
                lambda offset: data_refs[index].at[relative(offset), pl.ds(first_row, rows)],
                offset,
            )

    for offset in range(1, size, 2):
        for index in range(count):
            multiply(offset, index)
        if offset > 1:
            start_first(offset - 2)

    def own_block(turn, carry):
        for index in range(count):
            multiply(2 * turn, index)
        return carry

    own_block(0, 0)
    start_first(size - 1)
    lax.fori_loop(1, size // 2, own_block, 0)
    for stage in range(1, len(masks)):
        for item in range(len(items)):
            index, first_row, rows, order = items[item]
            for offset in received(item, stage - 1):
                copies[(item, offset)].wait_recv()
            for offset in received(item, stage):

                def store(index, at, value, offset=offset):
                    sums_refs[index][offset // 2 - 1, at, :] = value.astype(jnp.bfloat16)

                add_up(item, stage, offset, store)
            start(
                item,
                stage,
                lambda offset: sums_refs[index].at[offset // 2 - 1, pl.ds(first_row, rows)],
            )
    for item in range(len(items)):
        for offset in received(item, len(masks) - 1):
            copies[(item, offset)].wait_recv()

        def store_out(index, at, value):
            out_refs[index][at, :] = value

        add_up(item, len(masks), 0, store_out)
    for copy in copies.values():
        copy.wait_send()


def reduce_products(lhs, rhs, lefts, size, collective_id, splits=2):
    depth, model_width = lhs[0].shape
    rows = model_width // size
    widths = [array.shape[1] for array in rhs]
    count = len(rhs)
    items = count * splits
    return pl.pallas_call(
        functools.partial(reduce_kernel, size, splits, count, lefts, len(lhs)),
        out_shape=[jax.ShapeDtypeStruct((rows, width), jnp.float32) for width in widths],
        in_specs=[pl.BlockSpec(memory_space=pltpu.VMEM)] * (len(lhs) + count),
        out_specs=[pl.BlockSpec(memory_space=pltpu.VMEM)] * count,
        scratch_shapes=[pltpu.VMEM((size, rows, width), jnp.bfloat16) for width in widths]
        + [pltpu.VMEM((size - 1, rows, width), jnp.bfloat16) for width in widths]
        + [pltpu.VMEM((size // 2 - 1, rows, width), jnp.bfloat16) for width in widths]
        + [pltpu.SemaphoreType.DMA((items, size)), pltpu.SemaphoreType.DMA((items, size))],
        compiler_params=pltpu.CompilerParams(
            collective_id=collective_id, has_side_effects=True, vmem_limit_bytes=KERNEL_VMEM
        ),
        cost_estimate=pl.CostEstimate(
            flops=2 * depth * model_width * sum(widths),
            bytes_accessed=2 * model_width * sum(widths),
            transcendentals=0,
        ),
        name=f"reduce_products_{collective_id}",
    )(*lhs, *rhs)


def normalize(raw_in):
    return raw_in * lax.rsqrt(jnp.mean(raw_in * raw_in, axis=-1, keepdims=True) + EPSILON)


def norm_back(grad_normed, raw_in, gain_vec):
    factor = lax.rsqrt(jnp.mean(raw_in * raw_in, axis=-1, keepdims=True) + EPSILON)
    unit_rows = raw_in * factor
    scaled = grad_normed * gain_vec
    grad_raw = factor * (scaled - unit_rows * jnp.mean(scaled * unit_rows, axis=-1, keepdims=True))
    return (grad_raw, jnp.sum(grad_normed * unit_rows, axis=tuple(range(raw_in.ndim - 1))))


def rotate(values, cosine_tab, sine_tab, sign):
    half_size = values.shape[-1] // 2
    first_half = values[..., :half_size]
    second_half = values[..., half_size:]
    return jnp.concatenate(
        [
            first_half * cosine_tab - sign * second_half * sine_tab,
            second_half * cosine_tab + sign * first_half * sine_tab,
        ],
        axis=-1,
    )


def doc_layout(lengths, row_count):
    doc_ends = jnp.cumsum(lengths)
    token_index = jnp.arange(row_count, dtype=jnp.int32)
    past_end = (token_index[:, None] >= doc_ends[None, :]).astype(jnp.int32)
    doc_id = jnp.sum(past_end, axis=1)
    doc_pos = token_index - jnp.sum(past_end * lengths[None, :], axis=1)
    return (doc_id, doc_pos, token_index)


def rope_table(doc_pos, head_size):
    rope_freq = jnp.exp(
        jnp.arange(head_size // 2, dtype=jnp.float32) * (-2.0 * math.log(ROPE_BASE) / head_size)
    )
    rope_angle = doc_pos.astype(jnp.float32)[:, None] * rope_freq[None, :]
    return (jnp.cos(rope_angle)[:, None, :], jnp.sin(rope_angle)[:, None, :])


def shards(
    tokens,
    doc_lengths,
    slot_live,
    attn_gain,
    w_query,
    w_keyval,
    q_gain,
    k_gain,
    w_out,
    ffn_gain,
    w_gate,
    w_up,
    w_down,
    out_grad,
):
    row_count, model_width = tokens.shape
    head_size = q_gain.shape[0]
    heads_dev = w_query.shape[1] // head_size
    heads_all = heads_dev * lax.axis_size("mp")
    kv_heads = w_keyval.shape[1] // (2 * head_size)
    group_size = heads_all // kv_heads
    mp_size = lax.axis_size("mp")
    dp_size = lax.axis_size("dp")
    kv_window = max(
        ((index + 1) * heads_dev - 1) // group_size - (index * heads_dev) // group_size + 1
        for index in range(mp_size)
    )
    window_firsts = [
        min(index * heads_dev // group_size, kv_heads - kv_window) for index in range(mp_size)
    ]
    tile_cols = w_gate.shape[1] // slot_live.shape[0]
    shard_rows = row_count // lax.axis_size("mp")
    block_rows = min(512, row_count)
    score_scale = head_size ** (-0.5)
    head_span = heads_dev * head_size
    mp_index = lax.axis_index("mp")
    row_first = mp_index * shard_rows
    q_first = mp_index * heads_dev
    kv_first = jnp.minimum(q_first // group_size, kv_heads - kv_window)
    kv_owner = (q_first + jnp.arange(heads_dev, dtype=jnp.int32)) // group_size - kv_first
    head_pick = (kv_owner[:, None] == jnp.arange(kv_window, dtype=jnp.int32)[None, :]).astype(
        jnp.float32
    )
    key_cols = lax.dynamic_slice_in_dim(w_keyval, kv_first * head_size, kv_window * head_size, 1)
    value_cols = lax.dynamic_slice_in_dim(
        w_keyval, (kv_heads + kv_first) * head_size, kv_window * head_size, 1
    )

    def fold_heads(per_head):
        return jnp.einsum(
            "the,hw->twe",
            per_head.astype(jnp.bfloat16),
            head_pick.astype(jnp.bfloat16),
            preferred_element_type=jnp.float32,
        ).reshape(row_count, kv_window * head_size)

    def unfold_windows(per_source):
        sums = [None] * kv_heads
        for index, first in enumerate(window_firsts):
            for place in range(kv_window):
                part = per_source[index][:, place * head_size : (place + 1) * head_size].astype(
                    jnp.float32
                )
                head = first + place
                sums[head] = part if sums[head] is None else sums[head] + part
        return jnp.concatenate(sums, axis=1)

    dp_index = lax.axis_index("dp")
    out_piece = lax.dynamic_slice_in_dim(
        w_out, dp_index * (head_span // dp_size), head_span // dp_size, 0
    )
    w_out_full = lax.all_gather(out_piece, ("mp", "dp"), axis=0, tiled=True)
    doc_id, doc_pos, token_index = doc_layout(doc_lengths[0], row_count)
    cosine_tab, sine_tab = rope_table(doc_pos, head_size)
    x_float = tokens.astype(jnp.float32)
    x_rows = lax.dynamic_slice_in_dim(tokens, row_first, shard_rows, 0).astype(jnp.float32)
    gain_one = attn_gain.astype(jnp.float32)
    gain_two = ffn_gain.astype(jnp.float32)
    q_gain_f = q_gain.astype(jnp.float32)
    k_gain_f = k_gain.astype(jnp.float32)
    xn_one = (normalize(x_float) * gain_one).astype(jnp.bfloat16)
    q_raw = jnp.dot(xn_one, w_query, preferred_element_type=jnp.float32).reshape(
        row_count, heads_dev, head_size
    )
    kv_raw = jnp.dot(
        xn_one, jnp.concatenate([key_cols, value_cols], axis=1), preferred_element_type=jnp.float32
    ).reshape(row_count, 2, kv_window, head_size)
    k_raw = jnp.einsum("twe,hw->the", kv_raw[:, 0], head_pick, precision=HIGHEST_PREC)
    v_raw = jnp.einsum("twe,hw->the", kv_raw[:, 1], head_pick, precision=HIGHEST_PREC)
    q_rot = rotate(normalize(q_raw) * q_gain_f, cosine_tab, sine_tab, 1.0).astype(jnp.bfloat16)
    k_rot = rotate(normalize(k_raw) * k_gain_f, cosine_tab, sine_tab, 1.0).astype(jnp.bfloat16)
    v_low = v_raw.astype(jnp.bfloat16)

    def block_scores(row_start, key_stop):
        scores = (
            jnp.einsum(
                "qhe,khe->hqk",
                q_rot[row_start : row_start + block_rows],
                k_rot[:key_stop],
                preferred_element_type=jnp.float32,
            )
            * score_scale
        )
        allowed = (doc_id[row_start : row_start + block_rows, None] == doc_id[None, :key_stop]) & (
            token_index[None, :key_stop] <= token_index[row_start : row_start + block_rows, None]
        )
        return jnp.where(allowed[None], scores, MASKED)

    block_outs = []
    block_lse = []
    for row_start in range(0, row_count, block_rows):
        key_stop = row_start + block_rows
        scores = block_scores(row_start, key_stop)
        row_max = jnp.max(scores, axis=-1, keepdims=True)
        shifted = jnp.exp(scores - row_max)
        row_total = jnp.sum(shifted, axis=-1, keepdims=True)
        attn_probs = (shifted / row_total).astype(jnp.bfloat16)
        block_outs.append(
            jnp.einsum(
                "hqk,khe->qhe", attn_probs, v_low[:key_stop], preferred_element_type=jnp.float32
            )
        )
        block_lse.append(row_max + jnp.log(row_total))
    attended = (
        jnp.concatenate(block_outs, axis=0).reshape(row_count, head_span).astype(jnp.bfloat16)
    )
    att_rows_all = exchange(attended.reshape(mp_size, shard_rows, head_span), 1)
    att_rows_cat = jnp.concatenate([att_rows_all[i] for i in range(mp_size)], axis=1)
    hidden_rows = x_rows + jnp.dot(att_rows_cat, w_out_full, preferred_element_type=jnp.float32)
    chunks = 2
    chunk_rows = shard_rows // chunks
    xn_two_rows = (normalize(hidden_rows) * gain_two).astype(jnp.bfloat16)
    grad_chunks = out_grad.reshape(mp_size, chunks, chunk_rows, model_width)
    live_cols = jnp.repeat(slot_live.astype(jnp.float32), tile_cols)
    pieces = []
    for chunk in range(chunks):
        xn_two = lax.all_gather(
            xn_two_rows[chunk * chunk_rows : (chunk + 1) * chunk_rows], "mp", axis=0, tiled=True
        )
        if chunk:
            xn_two, _ = lax.optimization_barrier((xn_two, dn_two_low))
        grad_chunk = grad_chunks[:, chunk].reshape(mp_size * chunk_rows, model_width)
        gate_act = jnp.dot(xn_two, w_gate, preferred_element_type=jnp.float32)
        up_act = jnp.dot(xn_two, w_up, preferred_element_type=jnp.float32)
        gate_sigmoid = jax.nn.sigmoid(gate_act)
        gate_silu = gate_act * gate_sigmoid
        ffn_hidden = (gate_silu * up_act * live_cols).astype(jnp.bfloat16)
        d_hidden = (
            lax.dot_general(grad_chunk, w_down, CONTRACT_LAST, preferred_element_type=jnp.float32)
            * live_cols
        )
        d_gate = (
            d_hidden * up_act * gate_sigmoid * (1.0 + gate_act * (1.0 - gate_sigmoid))
        ).astype(jnp.bfloat16)
        d_up = (d_hidden * gate_silu).astype(jnp.bfloat16)
        dn_two_part = lax.dot_general(
            d_gate, w_gate, CONTRACT_LAST, preferred_element_type=jnp.float32
        ) + lax.dot_general(d_up, w_up, CONTRACT_LAST, preferred_element_type=jnp.float32)
        dn_two_low = dn_two_part.astype(jnp.bfloat16)
        dn_two_chunk = lax.psum_scatter(dn_two_low, "mp", scatter_dimension=0, tiled=True)
        pieces.append((xn_two, grad_chunk, ffn_hidden, d_gate, d_up, dn_two_chunk))
    xn_two, grad_cat, ffn_hidden, d_gate, d_up, dn_two_rows = (
        jnp.concatenate(parts, axis=0) for parts in zip(*pieces)
    )
    ffn_hidden, _ = lax.optimization_barrier((ffn_hidden, dn_two_low))
    ffn_part = jnp.dot(ffn_hidden, w_down, preferred_element_type=jnp.float32).astype(jnp.bfloat16)
    out_chunks = [
        lax.psum_scatter(part, "mp", scatter_dimension=0, tiled=True)
        for part in jnp.split(ffn_part, chunks, axis=0)
    ]
    xn_two, _ = lax.optimization_barrier((xn_two, ffn_part))
    grad_gate, grad_up, grad_down = reduce_products(
        (xn_two, grad_cat), (d_gate, d_up, ffn_hidden), (0, 0, 1), dp_size, 2
    )
    grad_down = grad_down.T
    dn_two_rows, grad_up = lax.optimization_barrier((dn_two_rows, grad_up))
    dn_two_rows = dn_two_rows.astype(jnp.float32)
    back_two, grad_gain_two = norm_back(dn_two_rows, hidden_rows, gain_two)
    g_rows = lax.dynamic_slice_in_dim(out_grad, row_first, shard_rows, 0)
    dh_rows = g_rows.astype(jnp.float32) + back_two
    dh_rows_low = dh_rows.astype(jnp.bfloat16)
    d_att_rows = lax.dot_general(
        dh_rows_low, w_out_full, CONTRACT_LAST, preferred_element_type=jnp.float32
    ).astype(jnp.bfloat16)
    d_att_blocks = jnp.stack(
        [d_att_rows[:, i * head_span : (i + 1) * head_span] for i in range(mp_size)]
    )
    d_att = exchange(d_att_blocks, 3)
    dh_low, _, out_chunks = lax.optimization_barrier((dh_rows_low, d_att, out_chunks))
    dh_low = lax.all_gather(dh_low, "mp", axis=0, tiled=True)
    d_att = d_att.reshape(row_count, heads_dev, head_size)
    dq_blocks = []
    d_keys = jnp.zeros((row_count, heads_dev, head_size), jnp.float32)
    d_values = jnp.zeros((row_count, heads_dev, head_size), jnp.float32)
    for block_index, row_start in enumerate(range(0, row_count, block_rows)):
        key_stop = row_start + block_rows
        scores = block_scores(row_start, key_stop)
        attn_probs = jnp.exp(scores - block_lse[block_index])
        probs_low = attn_probs.astype(jnp.bfloat16)
        att_rows = d_att[row_start:key_stop]
        d_probs = jnp.einsum(
            "qhe,khe->hqk", att_rows, v_low[:key_stop], preferred_element_type=jnp.float32
        )
        d_scores = (
            attn_probs * (d_probs - jnp.sum(d_probs * attn_probs, axis=-1, keepdims=True))
        ).astype(jnp.bfloat16)
        dq_blocks.append(
            jnp.einsum(
                "hqk,khe->qhe", d_scores, k_rot[:key_stop], preferred_element_type=jnp.float32
            )
            * score_scale
        )
        d_keys = d_keys.at[:key_stop].add(
            jnp.einsum(
                "hqk,qhe->khe",
                d_scores,
                q_rot[row_start:key_stop],
                preferred_element_type=jnp.float32,
            )
            * score_scale
        )
        d_values = d_values.at[:key_stop].add(
            jnp.einsum("hqk,qhe->khe", probs_low, att_rows, preferred_element_type=jnp.float32)
        )
    d_queries = jnp.concatenate(dq_blocks, axis=0)
    dq_raw, grad_q_gain = norm_back(rotate(d_queries, cosine_tab, sine_tab, -1.0), q_raw, q_gain_f)
    dk_raw, grad_k_gain = norm_back(rotate(d_keys, cosine_tab, sine_tab, -1.0), k_raw, k_gain_f)
    dq_low = dq_raw.reshape(row_count, head_span).astype(jnp.bfloat16)
    d_window = jnp.concatenate([fold_heads(dk_raw), fold_heads(d_values)], axis=1).astype(
        jnp.bfloat16
    )
    window_span = kv_window * head_size
    dn_one_part = (
        lax.dot_general(dq_low, w_query, CONTRACT_LAST, preferred_element_type=jnp.float32)
        + lax.dot_general(
            d_window,
            jnp.concatenate([key_cols, value_cols], axis=1),
            CONTRACT_LAST,
            preferred_element_type=jnp.float32,
        )
    ).astype(jnp.bfloat16)
    dn_one_rows = lax.psum_scatter(dn_one_part, "mp", scatter_dimension=0, tiled=True).astype(
        jnp.float32
    )
    back_one, grad_gain_one = norm_back(dn_one_rows, x_rows, gain_one)
    grad_tokens = dh_rows + back_one
    xn_one, _ = lax.optimization_barrier((xn_one, dn_one_part))
    grad_out_proj, grad_query, grad_window = reduce_products(
        (dh_low, xn_one), (attended, dq_low, d_window), (0, 1, 1), dp_size, 5
    )
    grad_out_proj = grad_out_proj.T
    window_rows = exchange(
        grad_window.astype(jnp.bfloat16).reshape(mp_size, -1, 2 * window_span), 6
    )
    grad_keyval = jnp.concatenate(
        [
            unfold_windows(window_rows[:, :, :window_span]),
            unfold_windows(window_rows[:, :, window_span:]),
        ],
        axis=1,
    )
    out_rows = hidden_rows + jnp.concatenate(out_chunks, axis=0).astype(jnp.float32)
    block_out = out_rows.astype(jnp.bfloat16)
    gain_sizes = (model_width, model_width, head_size, head_size)
    gains = jnp.concatenate([grad_gain_one, grad_gain_two, grad_q_gain, grad_k_gain])
    gain_rows = 8 * pl.cdiv(gains.shape[0], 1024)
    gains = jnp.pad(gains, (0, gain_rows * 128 - gains.shape[0])).reshape(gain_rows, 128)
    gains = sum_everywhere(gains, 7).reshape(-1)
    bounds = [sum(gain_sizes[:i]) for i in range(5)]
    grad_gain_one, grad_gain_two, grad_q_gain, grad_k_gain = (
        gains[bounds[i] : bounds[i + 1]] for i in range(4)
    )
    return (
        block_out,
        grad_tokens,
        grad_gain_one,
        grad_query,
        grad_keyval,
        grad_q_gain,
        grad_k_gain,
        grad_out_proj,
        grad_gain_two,
        grad_gate,
        grad_up,
        grad_down,
    )


def solution(mesh):
    return jax.shard_map(
        shards,
        mesh=mesh,
        in_specs=(
            P("dp", None),
            P("dp", None),
            P("mp"),
            P(),
            P(None, "mp"),
            P(),
            P(),
            P(),
            P("mp", None),
            P(),
            P(None, "mp"),
            P(None, "mp"),
            P("mp", None),
            P("dp", None),
        ),
        out_specs=(
            P(("dp", "mp"), None),
            P(("dp", "mp"), None),
            P(),
            P("dp", "mp"),
            P(("dp", "mp"), None),
            P(),
            P(),
            P("mp", "dp"),
            P(),
            P("dp", "mp"),
            P("dp", "mp"),
            P("mp", "dp"),
        ),
        check_vma=False,
    )
```
